32 devices in a mesh: rays: 2 (over x), freq: 16 (over z, y, core).
Axes of the slice: x: 2, y: 2, z: 4, core: 2. Of those that a mesh axis runs over, the one named last changes fastest.
Arguments:
- spectra: bfloat16 [32, 2, 1024, 1024], P(('rays', 'freq')), parts along dimension 0, may hold values from -6 to 6
- wavelet: float32 [16, 2], P('freq'), may hold values from -6 to 6
- freq_index: int32 [16], P('freq'), may hold values from 0 to 15, each once
- slowness: float32 [16], replicated, may hold values from 0.000222 to 0.000667
- layer_ids: int32 [1], replicated, may hold values from 0 to 15
- ray_slowness: float32 [4], P('rays'), parts along dimension 0, may hold values from -0.0001 to 0.0001
Outputs:
- migrated_image: float32 [2, 1024, 1024], P('rays', 'freq'), parts along dimension 0
The draws below stay inside these ranges and needn't reach their ends.
There are 2 independent parts, one for each index of `rays`. The reference program is written for one: setup_inputs(seed, part) draws one part's arguments, and reference() takes and returns one part's arrays. A program takes and returns all parts, laid end to end along the dimension named above; an argument that names none is the same for every part. Nothing has to cross between parts.
Inputs may be any that keep to these rules, and one draw needn't show every extreme that they name: `freq_index`: each frequency 0 to 15 is held by exactly one slot.
All inputs are finite; a program needn't handle non-finite values.
Results may differ from the reference program's by a relative error of at most 0.0065.
Values sent between devices are 32-bit elements; how exact they have to be, the bound alone decides.
A program may use at most 128 MiB of HBM per device.

```python
import math
import jax
import jax.numpy as jnp
from jax import lax

NX = 1024
NY = 1024
DEPTHS = 1
LAYERS = 16
FREQS = 16


def levels(own_key, extent, shards, smallest, high):
    gain = 1.0
    for dim, parts in shards:
        heights = jax.random.uniform(jax.random.fold_in(jax.random.fold_in(own_key, 6), dim), (parts,), jnp.float32, smallest / len(shards), high / len(shards))
        gain = gain * jnp.repeat(jnp.exp(heights), extent[dim] // parts).reshape((-1,) + (1,) * (len(extent) - 1 - dim))
    return gain


def normal_values(stream_key, extent, width, limit, pieces=(), kind=jnp.bfloat16):
    loudness = levels(stream_key, extent, pieces, -0.22, 0.18) if pieces else 1.0
    drawn = jax.random.normal(stream_key, extent, jnp.float32) * width * loudness
    return jnp.minimum(jnp.maximum(drawn, -limit), limit).astype(kind)


def setup_inputs(seed: int = 0, part: int = 0) -> dict:
    streams_of = jax.random.split(jax.random.key(seed), 7)
    own_keys = jax.random.split(jax.random.fold_in(streams_of[6], part), 7)
    spectra = normal_values(own_keys[0], (FREQS, 2, NY, NX), 1.0, 6.0, ((0, 16),))
    wavelet = normal_values(streams_of[1], (FREQS, 2), 1.0, 6.0, ((0, 16),), jnp.float32)
    freq_index = jax.random.permutation(streams_of[2], FREQS).astype(jnp.int32)
    slowness = jnp.clip(jnp.exp(jax.random.uniform(streams_of[3], (LAYERS,), jnp.float32, math.log(0.000222), math.log(0.000667))), 0.000222, 0.000667)
    layer_ids = jax.random.randint(streams_of[4], (DEPTHS,), 0, LAYERS).astype(jnp.int32)
    ray_slowness = jnp.clip(jax.random.uniform(own_keys[5], (2,), jnp.float32, -0.0001, 0.0001), -0.0001, 0.0001)
    return {"spectra": spectra, "wavelet": wavelet, "freq_index": freq_index, "slowness": slowness, "layer_ids": layer_ids, "ray_slowness": ray_slowness}


GRID_STEP = 12.5
DEPTH_STEP = 10.0
LOW_FREQUENCY = 5.0
FREQUENCY_BAND = 50.0
DAMPING = 6.0
radix_factor = 8

def block_table(length):
    left_side = jnp.arange(length, dtype=jnp.int32)[:, None]
    right_side = jnp.arange(length, dtype=jnp.int32)[None, :]
    angles = (left_side * right_side % length).astype(jnp.float32) * (2.0 * math.pi / length)
    cosines = jnp.cos(angles)
    sines = jnp.sin(angles)
    from_real = jnp.stack([cosines, sines], axis=1)
    from_imag = jnp.stack([-sines, cosines], axis=1)
    return jnp.stack([from_real, from_imag], axis=0).astype(jnp.bfloat16).astype(jnp.float32)

def twiddle(length):
    outer_pos = jnp.arange(radix_factor, dtype=jnp.int32)[:, None]
    inner_pos = jnp.arange(length // radix_factor, dtype=jnp.int32)[None, :]
    angles = (outer_pos * inner_pos % length).astype(jnp.float32) * (2.0 * math.pi / length)
    return (jnp.cos(angles), jnp.sin(angles))

def inverse_rows(field, small_table, large_table, twists):
    row_total = field.shape[1]
    column_total = field.shape[2]
    shaped = field.reshape(2, radix_factor, row_total // radix_factor, column_total).astype(jnp.float32)
    initial = jnp.einsum('cakx,cadn->dnkx', shaped, small_table, precision=lax.Precision.HIGHEST)
    cosines, sines = twists
    real_part = initial[0] * cosines[:, :, None] - initial[1] * sines[:, :, None]
    imag_part = initial[0] * sines[:, :, None] + initial[1] * cosines[:, :, None]
    turned = jnp.stack([real_part, imag_part]).astype(jnp.bfloat16).astype(jnp.float32)
    second = jnp.einsum('cnkx,ckdm->dmnx', turned, large_table, precision=lax.Precision.HIGHEST)
    return second.reshape(2, row_total, column_total).astype(jnp.bfloat16)

def inverse_columns(field, small_table, large_table, twists):
    row_total = field.shape[1]
    column_total = field.shape[2]
    shaped = field.reshape(2, row_total, radix_factor, column_total // radix_factor).astype(jnp.float32)
    initial = jnp.einsum('crak,cadn->drnk', shaped, small_table, precision=lax.Precision.HIGHEST)
    cosines, sines = twists
    real_part = initial[0] * cosines[None] - initial[1] * sines[None]
    imag_part = initial[0] * sines[None] + initial[1] * cosines[None]
    turned = jnp.stack([real_part, imag_part]).astype(jnp.bfloat16).astype(jnp.float32)
    second = jnp.einsum('crnk,ckdm->drmn', turned, large_table, precision=lax.Precision.HIGHEST)
    return second.reshape(2, row_total, column_total)

def wavenumbers(length):
    positions = jnp.arange(length, dtype=jnp.int32)
    signed = jnp.where(positions >= length // 2, positions - length, positions)
    return signed.astype(jnp.float32) * (2.0 * math.pi / (length * GRID_STEP))

def phase_factor(angular, layer_slow, wave_square):
    real_arg = (angular * angular - DAMPING * DAMPING) * layer_slow * layer_slow - wave_square
    imag_arg = 2.0 * angular * DAMPING * layer_slow * layer_slow
    modulus = jnp.sqrt(real_arg * real_arg + imag_arg * imag_arg)
    larger = jnp.sqrt(0.5 * (modulus + jnp.abs(real_arg)))
    smaller = imag_arg / (2.0 * larger)
    vertical_real = jnp.where(real_arg >= 0.0, larger, smaller)
    vertical_imag = jnp.where(real_arg >= 0.0, smaller, larger)
    damping_factor = jnp.exp(-vertical_imag * DEPTH_STEP)
    return (damping_factor * jnp.cos(vertical_real * DEPTH_STEP), damping_factor * jnp.sin(vertical_real * DEPTH_STEP))

def layer_value(slowness, layer_id):
    matches = jnp.arange(slowness.shape[0], dtype=jnp.int32) == layer_id
    return jnp.sum(jnp.where(matches, slowness, jnp.float32(0.0)))

def reference(spectra, wavelet, freq_index, slowness, layer_ids, ray_slowness):
    wave_y = wavenumbers(NY)
    wave_x = wavenumbers(NX)
    wave_square = wave_y[:, None] * wave_y[:, None] + wave_x[None, :] * wave_x[None, :]
    small_table = block_table(radix_factor)
    row_table = block_table(NY // radix_factor)
    column_table = block_table(NX // radix_factor)
    row_twists = twiddle(NY)
    column_twists = twiddle(NX)
    layer_slows = []
    delays = []
    delay_time = jnp.float32(0.0)
    for depth_level in range(DEPTHS):
        layer_slow = layer_value(slowness, layer_ids[depth_level])
        vertical = jnp.sqrt(layer_slow * layer_slow - ray_slowness[0] * ray_slowness[0] - ray_slowness[1] * ray_slowness[1])
        delay_time = delay_time + vertical * DEPTH_STEP
        layer_slows.append(layer_slow)
        delays.append(delay_time)
    column_place = jnp.arange(NX, dtype=jnp.int32).astype(jnp.float32) * GRID_STEP
    row_place = jnp.arange(NY, dtype=jnp.int32).astype(jnp.float32) * GRID_STEP

    def per_frequency(running, inputs):
        images, energies = running
        spectrum_in, wave_pair, position = inputs
        angular = (position.astype(jnp.float32) * (FREQUENCY_BAND / FREQS) + LOW_FREQUENCY) * (2.0 * math.pi)
        spectrum = spectrum_in.astype(jnp.float32)
        for depth_level in range(DEPTHS):
            cos_part, sin_part = phase_factor(angular, layer_slows[depth_level], wave_square)
            real_new = spectrum[0] * cos_part - spectrum[1] * sin_part
            imag_new = spectrum[0] * sin_part + spectrum[1] * cos_part
            spectrum = jnp.stack([real_new, imag_new])
            energies = energies.at[depth_level].add(jnp.sum(real_new * real_new + imag_new * imag_new))
            row_field = inverse_rows(spectrum.astype(jnp.bfloat16), small_table, row_table, row_twists)
            receiver = inverse_columns(row_field, small_table, column_table, column_twists)
            source_phase = angular * (ray_slowness[0] * column_place[None, :] + ray_slowness[1] * row_place[:, None] + delays[depth_level])
            cos_src = jnp.cos(source_phase)
            sin_src = jnp.sin(source_phase)
            weight_real = wave_pair[0] * cos_src + wave_pair[1] * sin_src
            weight_imag = wave_pair[0] * sin_src - wave_pair[1] * cos_src
            images = images.at[depth_level].add(weight_real * receiver[0] - weight_imag * receiver[1])
        return ((images, energies), None)
    start = (jnp.zeros((DEPTHS, NY, NX), jnp.float32), jnp.zeros((DEPTHS,), jnp.float32))
    (images, energies), unused = lax.scan(per_frequency, start, (spectra, wavelet, freq_index))
    energy_scale = 1.0 / jnp.sqrt(energies / FREQS + 1e-06)
    return images * energy_scale[:, None, None]
```

```python
import contextlib
import functools
import math

import jax
import jax.numpy as jnp
from jax import lax
from jax.experimental import pallas as pl
from jax.experimental.pallas import tpu as pltpu
from jax.sharding import PartitionSpec as P

GRID_STEP = 12.5
DEPTH_STEP = 10.0
LOW_FREQUENCY = 5.0
FREQUENCY_BAND = 50.0
DAMPING = 6.0
X_RADIX = 8
LANES = 128
LAG = 2
DEPTH = 4
YTALL = 64
EARLY = 2
MESH = pl.DeviceIdType.MESH

HALF_SIN = (0.9999998807907104, -0.16666465997695923, 0.008326363749802113, -0.00019062065985053778)
HALF_COS = (0.9999992251396179, -0.499982088804245, 0.04160428047180176, -0.0013190462486818433)
TURN_SIN = (0.9999992251396179, -0.16665679216384888, 0.008313224650919437, -0.0001852344867074862)
TURN_COS = (
    0.9999999403953552, -0.4999990463256836, 0.041663579642772675, -0.0013853666605427861,
    2.315317397005856e-05,
)

ROOT = math.sqrt(2.0)
PHASE_SIN = tuple(ROOT * c / 2.0 ** (2 * k + 1) for k, c in enumerate(HALF_SIN))
PHASE_COS = tuple(ROOT * c / 4.0**k for k, c in enumerate(HALF_COS))


def scope(name):
    return contextlib.nullcontext()


def polynomial(coefs, square):
    value = square * coefs[-1] + coefs[-2]
    for coef in coefs[-3::-1]:
        value = value * square + coef
    return value


def half_sincos(half, sin_coefs, cos_coefs):
    square = half * half
    sine = polynomial(sin_coefs, square) * half
    twice = sine + sine
    return twice * polynomial(cos_coefs, square), 1.0 - twice * sine


def turn_sincos(turns):
    reduced = turns - jnp.floor(turns + 0.5)
    return half_sincos(reduced * math.pi, TURN_SIN, TURN_COS)


def butterfly(parts):
    count = len(parts)
    if count == 1:
        return parts
    even = butterfly(parts[0::2])
    odd = butterfly(parts[1::2])
    low, high = [], []
    for i in range(count // 2):
        er, ei = even[i]
        xr, xi = odd[i]
        if i == 0:
            tr, ti = xr, xi
        elif 4 * i == count:
            tr, ti = -xi, xr
        elif 8 * i == count:
            root = math.sqrt(0.5)
            tr, ti = (xr - xi) * root, (xr + xi) * root
        elif 8 * i == 3 * count:
            root = math.sqrt(0.5)
            tr, ti = (xr + xi) * -root, (xr - xi) * root
        else:
            c = math.cos(2 * math.pi * i / count)
            s = math.sin(2 * math.pi * i / count)
            tr, ti = xr * c - xi * s, xr * s + xi * c
        low.append((er + tr, ei + ti))
        high.append((er - tr, ei - ti))
    return low + high


def kernel(
    groups, radix, pieces, freq_total,
    wavelet, freq_index, slowness, layer_ids, rays, spec_hbm, out_ref,
    spec, zed, ytab, field, xtab, vecs, fac, image, core_in, pair_in, low_in, high_in, etile, eall,
    load_sem, core_s, core_r, pair_s, pair_r, low_s, low_r, high_s, high_r, e_s, e_r,
):
    rows = spec.shape[1] * spec.shape[2]
    cols = spec.shape[3]
    short = rows // radix
    lines = groups // 4
    me = lax.axis_index("freq")
    core = lax.rem(me, 2)
    pair = lax.rem(me // 2, 2)
    spot = me // 4
    core_peer = me + 1 - 2 * core
    pair_peer = me + 2 - 4 * pair

    barrier = pltpu.get_barrier_semaphore()

    def greet(i, carry):
        pl.semaphore_signal(
            barrier, inc=1, device_id={"freq": lax.rem(me + i, groups)}, device_id_type=MESH
        )
        return carry

    lax.fori_loop(1, groups, greet, 0)

    strips = short // 16
    tiles = cols // LANES

    def load(i):
        window = pl.ds(pl.multiple_of(i * 16, 16), 16)
        return pltpu.make_async_copy(
            spec_hbm.at[:, :, window, :], spec.at[:, :, window, :], load_sem.at[i]
        )

    def start_load(i, carry):
        load(i).start()
        return carry

    lax.fori_loop(0, strips, start_load, 0)

    hertz = freq_index[0, 0].astype(jnp.float32) * (FREQUENCY_BAND / freq_total) + LOW_FREQUENCY
    angular = hertz * (2.0 * math.pi)
    slow = slowness[layer_ids[0, 0]]
    slow_sq = slow * slow
    ray_x = rays[0]
    ray_y = rays[1]
    real_base = (angular * angular - DAMPING * DAMPING) * slow_sq
    imag_arg = 2.0 * angular * DAMPING * slow_sq
    turn_x = hertz * ray_x * GRID_STEP
    turn_y = hertz * ray_y * GRID_STEP
    vertical = jnp.full((YTALL, LANES), slow_sq - ray_x * ray_x - ray_y * ray_y, jnp.float32)
    turn_0 = jnp.sqrt(vertical) * (DEPTH_STEP * hertz)
    wave_re = wavelet[0, 0]
    wave_im = wavelet[0, 1]

    block = cols // X_RADIX
    place = lax.broadcasted_iota(jnp.int32, (X_RADIX, cols), 1)
    outer = lax.broadcasted_iota(jnp.int32, (X_RADIX, cols), 0)
    eighth = lax.rem(place * outer, X_RADIX).astype(jnp.float32) * (1.0 / X_RADIX)
    vec_sin, vec_cos = turn_sincos(eighth + place.astype(jnp.float32) * turn_x)
    vecs[0] = vec_cos
    vecs[1] = vec_sin

    width = cols // pieces
    deep = 32

    def x_table(p):
        at = pl.ds(pl.multiple_of(p * width, LANES), width)
        x = lax.broadcasted_iota(jnp.int32, (deep, width), 1) + p * width
        x = x.astype(jnp.float32) * (1.0 / cols)
        k = lax.broadcasted_iota(jnp.int32, (deep, width), 0)

        def strip_of(strip, carry):
            sine, cosine = turn_sincos((k + strip * deep).astype(jnp.float32) * x)
            for k1 in range(X_RADIX):
                vc = vecs[0, k1 : k1 + 1, at]
                vs = vecs[1, k1 : k1 + 1, at]
                row = pl.ds(pl.multiple_of(strip * deep + k1 * block, deep), deep)
                row_im = pl.ds(pl.multiple_of(strip * deep + k1 * block + cols, deep), deep)
                xtab[row, at] = (cosine * vc - sine * vs).astype(jnp.bfloat16)
                xtab[row_im, at] = (-(cosine * vs) - sine * vc).astype(jnp.bfloat16)
            return carry

        lax.fori_loop(0, block // deep, strip_of, 0, unroll=True)

    with scope("xt0"):
        x_table(0)

    ytiles = short // LANES

    tall = short // YTALL

    def y_table(step, carry):
        n1 = step // (tall * ytiles)
        strip = lax.rem(step // ytiles, tall)
        tile = lax.rem(step, ytiles)
        n2 = lax.broadcasted_iota(jnp.int32, (YTALL, LANES), 0) + strip * YTALL
        k2 = lax.broadcasted_iota(jnp.int32, (YTALL, LANES), 1) + tile * LANES
        n = n2 * radix + n1
        n = n.astype(jnp.float32)
        turns = k2.astype(jnp.float32) * (n * (1.0 / rows))
        turns = turns - jnp.floor(turns)
        sine, cosine = turn_sincos(turns + n * turn_y + turn_0)
        real = (wave_re * cosine + wave_im * sine).astype(jnp.bfloat16)
        imag_f = wave_re * sine - wave_im * cosine
        imag = imag_f.astype(jnp.bfloat16)
        top = pl.ds(pl.multiple_of(strip * YTALL, YTALL), YTALL)
        bottom = pl.ds(pl.multiple_of(strip * YTALL + short, YTALL), YTALL)
        left = pl.ds(pl.multiple_of(tile * LANES, LANES), LANES)
        right = pl.ds(pl.multiple_of(tile * LANES + short, LANES), LANES)
        ytab[n1, top, left] = real
        ytab[n1, top, right] = (-imag_f).astype(jnp.bfloat16)
        ytab[n1, bottom, left] = imag
        ytab[n1, bottom, right] = real
        return carry

    with scope("ytab"):
        lax.fori_loop(0, radix * tall * ytiles, y_table, 0, unroll=2)

    half_gain = 0.5 * DEPTH_STEP * DEPTH_STEP
    step_y = 2.0 * math.pi / (rows * GRID_STEP) * math.sqrt(half_gain)
    step_x = 2.0 * math.pi / (cols * GRID_STEP) * math.sqrt(half_gain)
    base = real_base * half_gain
    imag = imag_arg * half_gain
    imag_sq = imag * imag

    def factor(a):
        m = a * a + imag_sq
        q = m * lax.rsqrt(m) + jnp.abs(a)
        iq = lax.rsqrt(q)
        g = q * iq
        h = imag * iq
        forward = a >= 0.0
        vert_re = jnp.where(forward, g, h)
        vert_im = jnp.where(forward, h, g)
        damp = jnp.exp2(vert_im * -math.log2(math.e))
        square = vert_re * vert_re
        v = polynomial(PHASE_SIN, square) * vert_re
        w = polynomial(PHASE_COS, square)
        dv = damp * v
        return damp - dv * v, dv * w

    def signed(index, extent):
        return jnp.where(index >= extent // 2, index - extent, index).astype(jnp.float32)

    lane = lax.broadcasted_iota(jnp.int32, (16, LANES), 1)
    sub = lax.broadcasted_iota(jnp.int32, (16, LANES), 0)
    kx_sq = []
    for t in range(tiles // 2):
        kx = (lane + t * LANES).astype(jnp.float32) * step_x
        kx_sq.append(kx * kx)
    edge_y = signed(lane * 16 + sub, rows) * step_y
    edge_x = cols // 2 * step_x
    edge = factor(base - edge_x * edge_x - edge_y * edge_y)
    turned = lax.rem(LANES - lane, LANES)
    first = lane == 0

    def factors(m, carry):
        rows_at = pl.ds(pl.multiple_of(m * 16, 16), 16)
        ky = signed(sub + m * 16, rows) * step_y
        ybase = base - ky * ky
        here = jnp.full((16, LANES), m, jnp.int32)
        after = [jnp.take_along_axis(e, here, axis=1) for e in edge]
        for t in reversed(range(tiles // 2)):
            now = factor(ybase - kx_sq[t])
            for c in range(2):
                fac[c, rows_at, t * LANES : (t + 1) * LANES] = now[c]
                back = jnp.take_along_axis(now[c], turned, axis=1)
                far = tiles - 1 - t
                fac[c, rows_at, far * LANES : (far + 1) * LANES] = jnp.where(first, after[c], back)
            after = now
        return carry

    with scope("factors"):
        lax.fori_loop(0, rows // 16, factors, 0)

    def shift(strip, total):
        load(strip).wait()
        rows_at = pl.ds(pl.multiple_of(strip * 16, 16), 16)

        def inner(tile, acc):
            at = pl.ds(pl.multiple_of(tile * LANES, LANES), LANES)
            parts = []
            for k1 in range(radix):
                row = pl.ds(pl.multiple_of(strip * 16 + k1 * short, 16), 16)
                cosine = fac[0, row, at]
                sine = fac[1, row, at]
                re = spec[0, k1, rows_at, at].astype(jnp.float32)
                im = spec[1, k1, rows_at, at].astype(jnp.float32)
                new_re = re * cosine - im * sine
                new_im = re * sine + im * cosine
                acc = acc + (new_re * new_re + new_im * new_im)
                parts.append((new_re.astype(jnp.bfloat16), new_im.astype(jnp.bfloat16)))
            for n1, (re, im) in enumerate(butterfly(parts)):
                zed[n1, rows_at, at] = re
                low = pl.ds(pl.multiple_of(strip * 16 + short, 16), 16)
                zed[n1, low, at] = im
            return acc

        return lax.fori_loop(0, tiles, inner, total, unroll=2)

    with scope("shift"):
        energy = lax.fori_loop(0, strips, shift, jnp.zeros((16, LANES), jnp.float32))
    etile[...] = energy[:8] + energy[8:]

    chips = groups // 2

    def y_stage(n1, carry):
        for part in range(cols // 256):
            at = slice(part * 256, part * 256 + 256)
            at_im = slice(cols + part * 256, cols + part * 256 + 256)
            res = jnp.dot(ytab[n1], zed[n1, :, at], preferred_element_type=jnp.float32)
            res = res.astype(jnp.bfloat16)
            field[:, n1, :, at] = res[:short].reshape(chips, 16, 256)
            field[:, n1, :, at_im] = res[short:].reshape(chips, 16, 256)
        return carry

    with scope("ystage"):
        lax.fori_loop(0, radix, y_stage, 0, unroll=True)

    with scope("barr"):
        pl.semaphore_wait(barrier, groups - 1)

    def energy_copy(i):
        return pltpu.make_async_remote_copy(
            src_ref=etile, dst_ref=eall.at[i], send_sem=e_s.at[i], recv_sem=e_r.at[i],
            device_id={"freq": lax.rem(me + i, groups)}, device_id_type=MESH,
        )

    def energy_start(i, carry):
        energy_copy(i).start()
        return carry

    lax.fori_loop(1, groups, energy_start, 0)

    def order(j):
        half = j // 2
        return jnp.where(lax.rem(j, 2) == 0, half, lines - 1 - half)

    def cut_of(p):
        return pl.ds(pl.multiple_of(p * width, LANES), width)

    def core_copy(p, b):
        cut = cut_of(p)
        return pltpu.make_async_remote_copy(
            src_ref=image.at[:, b, 1 - core, :, :, cut], dst_ref=core_in.at[:, b, :, :, cut],
            send_sem=core_s.at[p, b], recv_sem=core_r.at[p, b],
            device_id={"freq": core_peer}, device_id_type=MESH,
        )

    def pair_copy(a, p):
        cut = cut_of(p)
        return pltpu.make_async_remote_copy(
            src_ref=image.at[a, 1 - pair, core, :, :, cut], dst_ref=pair_in.at[a, :, :, cut],
            send_sem=pair_s.at[a, p], recv_sem=pair_r.at[a, p],
            device_id={"freq": pair_peer}, device_id_type=MESH,
        )

    def low_copy(a, p):
        cut = cut_of(p)
        return pltpu.make_async_remote_copy(
            src_ref=image.at[a, pair, core, :, :, cut], dst_ref=low_in.at[a, :, :, cut],
            send_sem=low_s.at[a, p], recv_sem=low_r.at[a, p],
            device_id={"freq": jnp.minimum(spot + 1, lines - 1) * 4 + pair * 2 + core},
            device_id_type=MESH,
        )

    def high_copy(a, p):
        cut = cut_of(p)
        return pltpu.make_async_remote_copy(
            src_ref=image.at[a, pair, core, :, :, cut], dst_ref=high_in.at[a, :, :, cut],
            send_sem=high_s.at[a, p], recv_sem=high_r.at[a, p],
            device_id={"freq": jnp.maximum(spot - 1, 0) * 4 + pair * 2 + core},
            device_id_type=MESH,
        )

    count = lines * pieces
    depth = min(DEPTH, count)

    def split(i):
        return order(lax.rem(i, lines)), i // lines

    def first_of(i):
        return lax.rem(i, lines) == 0

    def send_pair(i):
        a, p = split(i)
        cut = cut_of(p)

        @pl.when(first_of(i))
        def _():
            core_copy(p, 1 - pair).wait_recv()

        image[a, 1 - pair, core, :, :, cut] = (
            image[a, 1 - pair, core, :, :, cut] + core_in[a, 1 - pair, :, :, cut]
        )
        pair_copy(a, p).start()

    def third(i, carry):
        @pl.when(i < count)
        def _():
            a, p = split(jnp.minimum(i, count - 1))
            cut = cut_of(p)
            pair_copy(a, p).wait_recv()

            @pl.when(i + depth < count)
            def _():
                send_pair(jnp.minimum(i + depth, count - 1))

            @pl.when(first_of(i))
            def _():
                core_copy(p, pair).wait_recv()

            image[a, pair, core, :, :, cut] = (
                image[a, pair, core, :, :, cut] + core_in[a, pair, :, :, cut] + pair_in[a, :, :, cut]
            )

        upward = i - LAG * spot
        a_up, p_up = split(jnp.clip(upward, 0, count - 1))

        @pl.when((upward >= 0) & (upward < count) & (a_up > spot))
        def _():
            cut = cut_of(p_up)

            @pl.when(spot > 0)
            def _():
                low_copy(a_up, p_up).wait_recv()
                image[a_up, pair, core, :, :, cut] = image[a_up, pair, core, :, :, cut] + low_in[a_up, :, :, cut]

            low_copy(a_up, p_up).start()

        downward = i - LAG * (lines - 1 - spot)
        a_dn, p_dn = split(jnp.clip(downward, 0, count - 1))

        @pl.when((downward >= 0) & (downward < count) & (a_dn < spot))
        def _():
            cut = cut_of(p_dn)

            @pl.when(spot < lines - 1)
            def _():
                high_copy(a_dn, p_dn).wait_recv()
                image[a_dn, pair, core, :, :, cut] = image[a_dn, pair, core, :, :, cut] + high_in[a_dn, :, :, cut]

            high_copy(a_dn, p_dn).start()

        return carry

    def compute(p, carry):
        at = cut_of(p)

        @pl.when(p > 0)
        def _():
            x_table(p)

        @pl.when(p == 1)
        def _():
            lax.fori_loop(0, depth, lambda i, c: (send_pair(i), c)[1], 0)

        lax.fori_loop(EARLY * jnp.maximum(p - 2, 0), EARLY * jnp.maximum(p - 1, 0), third, 0)

        half = max(lines // 4, 1)
        for q in range(lines // half):
            lhs = field[2 * half * q : 2 * half * (q + 1)].reshape(half * 2 * radix * 16, 2 * cols)
            res = jnp.dot(lhs, xtab[:, at], preferred_element_type=jnp.float32)
            res = res.reshape(half, 2, radix, 2, 8, width)
            for c in range(2):
                image[half * q : half * (q + 1), :, c, :, :, at] = res[:, :, :, c]
        core_copy(p, 1 - pair).start()
        core_copy(p, pair).start()
        return carry

    with scope("compute"):
        lax.fori_loop(0, pieces, compute, 0)

    with scope("third"):
        lax.fori_loop(EARLY * max(pieces - 2, 0), count + LAG * (lines - 1), third, 0)

    def energy_take(i, total):
        energy_copy(i).wait_recv()
        return total + eall[i]

    total = lax.fori_loop(1, groups, energy_take, etile[...])
    total = jnp.sum(jnp.sum(total, axis=0, keepdims=True), axis=1, keepdims=True)
    scale = lax.rsqrt(total / freq_total + 1e-06)

    def own(p, carry):
        cut = cut_of(p)

        @pl.when(spot > 0)
        def _():
            low_copy(spot, p).wait_recv()
            image[spot, pair, core, :, :, cut] = image[spot, pair, core, :, :, cut] + low_in[spot, :, :, cut]

        @pl.when(spot < lines - 1)
        def _():
            high_copy(spot, p).wait_recv()
            image[spot, pair, core, :, :, cut] = image[spot, pair, core, :, :, cut] + high_in[spot, :, :, cut]

        return carry

    with scope("own"):
        lax.fori_loop(0, pieces, own, 0)
    for n1 in range(radix):
        out_ref[:, n1, :] = image[spot, pair, core, n1] * scale

    def energy_end(i, carry):
        energy_copy(i).wait_send()
        return carry

    lax.fori_loop(1, groups, energy_end, 0)

    def finish_core(p, carry):
        core_copy(p, 0).wait_send()
        core_copy(p, 1).wait_send()
        return carry

    lax.fori_loop(0, pieces, finish_core, 0)

    def finish(a, carry):
        def piece(p, inner):
            pair_copy(a, p).wait_send()

            @pl.when(a > spot)
            def _():
                low_copy(a, p).wait_send()

            @pl.when(a < spot)
            def _():
                high_copy(a, p).wait_send()

            return inner

        return lax.fori_loop(0, pieces, piece, carry)

    lax.fori_loop(0, lines, finish, 0)


def body(spectra, wavelet, freq_index, slowness, layer_ids, ray_slowness):
    slot_total, unused, rows, cols = spectra.shape
    groups = lax.axis_size("freq")
    freq_total = slot_total * groups
    radix = rows // groups // 8
    short = rows // radix
    lines = groups // 4
    pieces = min(4, cols // LANES)
    f32, bf16 = jnp.float32, jnp.bfloat16
    dma = pltpu.SemaphoreType.DMA
    out = pl.pallas_call(
        functools.partial(kernel, groups, radix, pieces, freq_total),
        out_shape=jax.ShapeDtypeStruct((8, radix, cols), f32),
        in_specs=[
            *[pl.BlockSpec(memory_space=pltpu.SMEM)] * 5,
            pl.BlockSpec(memory_space=pl.ANY),
        ],
        out_specs=pl.BlockSpec(memory_space=pltpu.VMEM),
        scratch_shapes=[
            pltpu.VMEM((2, radix, short, cols), bf16),
            pltpu.VMEM((radix, 2 * short, cols), bf16),
            pltpu.VMEM((radix, 2 * short, 2 * short), bf16),
            pltpu.VMEM((groups // 2, radix, 16, 2 * cols), bf16),
            pltpu.VMEM((2 * cols, cols), bf16),
            pltpu.VMEM((2, X_RADIX, cols), f32),
            pltpu.VMEM((2, rows, cols), f32),
            pltpu.VMEM((lines, 2, 2, radix, 8, cols), f32),
            pltpu.VMEM((lines, 2, radix, 8, cols), f32),
            pltpu.VMEM((lines, radix, 8, cols), f32),
            pltpu.VMEM((lines, radix, 8, cols), f32),
            pltpu.VMEM((lines, radix, 8, cols), f32),
            pltpu.VMEM((8, LANES), f32),
            pltpu.VMEM((groups, 8, LANES), f32),
            dma((short // 16,)),
            dma((pieces, 2)),
            dma((pieces, 2)),
            dma((lines, pieces)),
            dma((lines, pieces)),
            dma((lines, pieces)),
            dma((lines, pieces)),
            dma((lines, pieces)),
            dma((lines, pieces)),
            dma((groups,)),
            dma((groups,)),
        ],
        compiler_params=pltpu.CompilerParams(
            collective_id=0, has_side_effects=True, vmem_limit_bytes=60 * 1024 * 1024
        ),
    )(
        wavelet, freq_index.reshape(1, 1), slowness, layer_ids.reshape(1, 1), ray_slowness,
        spectra.reshape(2, radix, short, cols),
    )
    return out.reshape(1, 8 * radix, cols)


def solution(mesh):
    placed = (
        P(("rays", "freq"), None, None, None),
        P("freq", None),
        P("freq"),
        P(),
        P(),
        P("rays"),
    )
    return jax.shard_map(
        body, mesh=mesh, in_specs=placed, out_specs=P("rays", "freq", None), check_vma=False
    )
```

```python
import contextlib
import functools
import math

import jax
import jax.numpy as jnp
from jax import lax
from jax.experimental import pallas as pl
from jax.experimental.pallas import tpu as pltpu
from jax.sharding import PartitionSpec as P

GRID_STEP = 12.5
DEPTH_STEP = 10.0
LOW_FREQUENCY = 5.0
FREQUENCY_BAND = 50.0
DAMPING = 6.0
LANES = 128
LAG = 2
BEHIND = 3
SKIP = 2
OWN = 4
YTALL = 64
MESH = pl.DeviceIdType.MESH

HALF_SIN = (0.9999998807907104, -0.16666465997695923, 0.008326363749802113, -0.00019062065985053778)
HALF_COS = (0.9999992251396179, -0.499982088804245, 0.04160428047180176, -0.0013190462486818433)
TURN_SIN = (0.9999992251396179, -0.16665679216384888, 0.008313224650919437, -0.0001852344867074862)
TURN_COS = (
    0.9999999403953552, -0.4999990463256836, 0.041663579642772675, -0.0013853666605427861,
    2.315317397005856e-05,
)

ROOT = math.sqrt(2.0)
PHASE_SIN = tuple(ROOT * c / 2.0 ** (2 * k + 1) for k, c in enumerate(HALF_SIN))
PHASE_COS = tuple(ROOT * c / 4.0**k for k, c in enumerate(HALF_COS))


def scope(name):
    return contextlib.nullcontext()


def polynomial(coefs, square):
    value = square * coefs[-1] + coefs[-2]
    for coef in coefs[-3::-1]:
        value = value * square + coef
    return value


def half_sincos(half, sin_coefs, cos_coefs):
    square = half * half
    sine = polynomial(sin_coefs, square) * half
    twice = sine + sine
    return twice * polynomial(cos_coefs, square), 1.0 - twice * sine


def turn_sincos(turns):
    reduced = turns - jnp.floor(turns + 0.5)
    return half_sincos(reduced * math.pi, TURN_SIN, TURN_COS)


def butterfly(parts):
    count = len(parts)
    if count == 1:
        return parts
    even = butterfly(parts[0::2])
    odd = butterfly(parts[1::2])
    low, high = [], []
    for i in range(count // 2):
        er, ei = even[i]
        xr, xi = odd[i]
        if i == 0:
            tr, ti = xr, xi
        elif 4 * i == count:
            tr, ti = -xi, xr
        elif 8 * i == count:
            root = math.sqrt(0.5)
            tr, ti = (xr - xi) * root, (xr + xi) * root
        elif 8 * i == 3 * count:
            root = math.sqrt(0.5)
            tr, ti = (xr + xi) * -root, (xr - xi) * root
        else:
            c = math.cos(2 * math.pi * i / count)
            s = math.sin(2 * math.pi * i / count)
            tr, ti = xr * c - xi * s, xr * s + xi * c
        low.append((er + tr, ei + ti))
        high.append((er - tr, ei - ti))
    return low + high


def kernel(
    groups, radix, pieces, freq_total,
    wavelet, freq_index, slowness, layer_ids, rays, spec_hbm, out_ref,
    spec, zed, ytab, field, xtab, yout, fac, image, core_in, pair_in, low_in, high_in, other_in, etile, eall,
    load_sem, core_s, core_r, pair_s, pair_r, low_s, low_r, high_s, high_r, other_s, other_r, e_s, e_r,
):
    rows = spec.shape[1] * spec.shape[2]
    cols = spec.shape[3]
    short = rows // radix
    lines = groups // 4
    me = lax.axis_index("freq")
    core = lax.rem(me, 2)
    pair = lax.rem(me // 2, 2)
    spot = me // 4
    core_peer = me + 1 - 2 * core
    pair_peer = me + 2 - 4 * pair

    barrier = pltpu.get_barrier_semaphore()

    def greet(i, carry):
        pl.semaphore_signal(
            barrier, inc=1, device_id={"freq": lax.rem(me + i, groups)}, device_id_type=MESH
        )
        return carry

    lax.fori_loop(1, groups, greet, 0)

    strips = short // 16
    tiles = cols // LANES

    def load(i):
        window = pl.ds(pl.multiple_of(i * 16, 16), 16)
        return pltpu.make_async_copy(
            spec_hbm.at[:, :, window, :], spec.at[:, :, window, :], load_sem.at[i]
        )

    def start_load(i, carry):
        load(i).start()
        return carry

    lax.fori_loop(0, strips, start_load, 0)

    hertz = freq_index[0, 0].astype(jnp.float32) * (FREQUENCY_BAND / freq_total) + LOW_FREQUENCY
    angular = hertz * (2.0 * math.pi)
    slow = slowness[layer_ids[0, 0]]
    slow_sq = slow * slow
    ray_x = rays[0]
    ray_y = rays[1]
    real_base = (angular * angular - DAMPING * DAMPING) * slow_sq
    imag_arg = 2.0 * angular * DAMPING * slow_sq
    turn_x = hertz * ray_x * GRID_STEP
    turn_y = hertz * ray_y * GRID_STEP
    vertical = jnp.full((YTALL, LANES), slow_sq - ray_x * ray_x - ray_y * ray_y, jnp.float32)
    turn_0 = jnp.sqrt(vertical) * (DEPTH_STEP * hertz)
    wave_re = wavelet[0, 0]
    wave_im = wavelet[0, 1]

    width = cols // pieces
    deep = 32

    def x_table(p):
        x = lax.broadcasted_iota(jnp.int32, (deep, width), 1) * pieces + p
        x = x.astype(jnp.float32)
        away = x * turn_x
        away = away - jnp.floor(away)
        x = x * (1.0 / cols)
        k = lax.broadcasted_iota(jnp.int32, (deep, width), 0)

        def strip_of(strip, carry):
            sine, cosine = turn_sincos((k + strip * deep).astype(jnp.float32) * x + away)
            row = pl.ds(pl.multiple_of(strip * deep, deep), deep)
            row_im = pl.ds(pl.multiple_of(strip * deep + width, deep), deep)
            xtab[p, row, :] = cosine.astype(jnp.bfloat16)
            xtab[p, row_im, :] = (-sine).astype(jnp.bfloat16)
            return carry

        lax.fori_loop(0, width // deep, strip_of, 0, unroll=True)

    with scope("xt0"):
        x_table(0)

    ytiles = short // LANES

    tall = short // YTALL

    def y_table(step, carry):
        n1 = step // (tall * ytiles)
        strip = lax.rem(step // ytiles, tall)
        tile = lax.rem(step, ytiles)
        n2 = lax.broadcasted_iota(jnp.int32, (YTALL, LANES), 0) + strip * YTALL
        k2 = lax.broadcasted_iota(jnp.int32, (YTALL, LANES), 1) + tile * LANES
        n = n2 * radix + n1
        n = n.astype(jnp.float32)
        turns = k2.astype(jnp.float32) * (n * (1.0 / rows))
        turns = turns - jnp.floor(turns)
        sine, cosine = turn_sincos(turns + n * turn_y + turn_0)
        real = (wave_re * cosine + wave_im * sine).astype(jnp.bfloat16)
        imag_f = wave_re * sine - wave_im * cosine
        imag = imag_f.astype(jnp.bfloat16)
        top = pl.ds(pl.multiple_of(strip * YTALL, YTALL), YTALL)
        bottom = pl.ds(pl.multiple_of(strip * YTALL + short, YTALL), YTALL)
        left = pl.ds(pl.multiple_of(tile * LANES, LANES), LANES)
        right = pl.ds(pl.multiple_of(tile * LANES + short, LANES), LANES)
        ytab[n1, top, left] = real
        ytab[n1, top, right] = (-imag_f).astype(jnp.bfloat16)
        ytab[n1, bottom, left] = imag
        ytab[n1, bottom, right] = real
        return carry

    with scope("ytab"):
        lax.fori_loop(0, radix * tall * ytiles, y_table, 0, unroll=2)

    half_gain = 0.5 * DEPTH_STEP * DEPTH_STEP
    step_y = 2.0 * math.pi / (rows * GRID_STEP) * math.sqrt(half_gain)
    step_x = 2.0 * math.pi / (cols * GRID_STEP) * math.sqrt(half_gain)
    base = real_base * half_gain
    imag = imag_arg * half_gain
    imag_sq = imag * imag

    def factor(a):
        m = a * a + imag_sq
        q = m * lax.rsqrt(m) + jnp.abs(a)
        iq = lax.rsqrt(q)
        g = q * iq
        h = imag * iq
        forward = a >= 0.0
        vert_re = jnp.where(forward, g, h)
        vert_im = jnp.where(forward, h, g)
        damp = jnp.exp2(vert_im * -math.log2(math.e))
        square = vert_re * vert_re
        v = polynomial(PHASE_SIN, square) * vert_re
        w = polynomial(PHASE_COS, square)
        dv = damp * v
        return damp - dv * v, dv * w

    def signed(index, extent):
        return jnp.where(index >= extent // 2, index - extent, index).astype(jnp.float32)

    lane = lax.broadcasted_iota(jnp.int32, (16, LANES), 1)
    sub = lax.broadcasted_iota(jnp.int32, (16, LANES), 0)
    kx_sq = []
    for t in range(tiles // 2):
        kx = (lane + t * LANES).astype(jnp.float32) * step_x
        kx_sq.append(kx * kx)
    edge_y = signed(lane * 16 + sub, rows) * step_y
    edge_x = cols // 2 * step_x
    edge = factor(base - edge_x * edge_x - edge_y * edge_y)
    turned = lax.rem(LANES - lane, LANES)
    first = lane == 0

    def factors(m, carry):
        rows_at = pl.ds(pl.multiple_of(m * 16, 16), 16)
        ky = signed(sub + m * 16, rows) * step_y
        ybase = base - ky * ky
        here = jnp.full((16, LANES), m, jnp.int32)
        after = [jnp.take_along_axis(e, here, axis=1) for e in edge]
        for t in reversed(range(tiles // 2)):
            now = factor(ybase - kx_sq[t])
            for c in range(2):
                fac[c, rows_at, t * LANES : (t + 1) * LANES] = now[c]
                back = jnp.take_along_axis(now[c], turned, axis=1)
                far = tiles - 1 - t
                fac[c, rows_at, far * LANES : (far + 1) * LANES] = jnp.where(first, after[c], back)
            after = now
        return carry

    with scope("factors"):
        lax.fori_loop(0, rows // 16, factors, 0, unroll=4)

    def shift(strip, total):
        load(strip).wait()
        rows_at = pl.ds(pl.multiple_of(strip * 16, 16), 16)

        def inner(tile, acc):
            at = pl.ds(pl.multiple_of(tile * LANES, LANES), LANES)
            parts = []
            for k1 in range(radix):
                row = pl.ds(pl.multiple_of(strip * 16 + k1 * short, 16), 16)
                cosine = fac[0, row, at]
                sine = fac[1, row, at]
                re = spec[0, k1, rows_at, at].astype(jnp.float32)
                im = spec[1, k1, rows_at, at].astype(jnp.float32)
                new_re = re * cosine - im * sine
                new_im = re * sine + im * cosine
                acc = acc + (new_re * new_re + new_im * new_im)
                parts.append((new_re.astype(jnp.bfloat16), new_im.astype(jnp.bfloat16)))
            for n1, (re, im) in enumerate(butterfly(parts)):
                zed[n1, rows_at, at] = re
                low = pl.ds(pl.multiple_of(strip * 16 + short, 16), 16)
                zed[n1, low, at] = im
            return acc

        return lax.fori_loop(0, tiles, inner, total, unroll=2)

    with scope("shift"):
        energy = lax.fori_loop(0, strips, shift, jnp.zeros((16, LANES), jnp.float32))
    etile[...] = energy[:8] + energy[8:]

    chips = groups // 2

    def y_stage(n1, carry):
        for part in range(pieces):
            at = slice(part * width, (part + 1) * width)
            yout[part] = jnp.dot(ytab[n1], zed[n1, :, at], preferred_element_type=jnp.float32)

        def fold(strip, inner):
            top = pl.ds(pl.multiple_of(strip * 16, 16), 16)
            low = pl.ds(pl.multiple_of(strip * 16 + short, 16), 16)
            for lane_tile in range(width // LANES):
                left = slice(lane_tile * LANES, (lane_tile + 1) * LANES)
                right = slice(width + lane_tile * LANES, width + (lane_tile + 1) * LANES)
                terms = [(yout[part, top, left], yout[part, low, left]) for part in range(pieces)]
                for x1, (re, im) in enumerate(butterfly(terms)):
                    field[x1, strip, n1, :, left] = re.astype(jnp.bfloat16)
                    field[x1, strip, n1, :, right] = im.astype(jnp.bfloat16)
            return inner

        lax.fori_loop(0, chips, fold, 0, unroll=True)
        return carry

    with scope("ystage"):
        lax.fori_loop(0, radix, y_stage, 0, unroll=True)

    with scope("barr"):
        pl.semaphore_wait(barrier, groups - 1)

    def energy_copy(i):
        return pltpu.make_async_remote_copy(
            src_ref=etile, dst_ref=eall.at[i], send_sem=e_s.at[i], recv_sem=e_r.at[i],
            device_id={"freq": lax.rem(me + i, groups)}, device_id_type=MESH,
        )

    def energy_start(i, carry):
        energy_copy(i).start()
        return carry

    lax.fori_loop(1, groups, energy_start, 0)

    def ranked(j, count, centre):
        up = count - 1 - centre
        near = jnp.minimum(up, centre)
        lead = jnp.maximum(up, centre) - near
        sign = jnp.where(up >= centre, 1, -1)
        rest = jnp.maximum(j - lead, 0)
        side = jnp.where(lax.rem(rest, 2) == 0, sign, -sign)
        return jnp.where(j < lead, centre + sign * (lead + near - j), centre + side * (near - rest // 2))

    half = max(lines // 4, 1)
    blocks = lines // half
    away = (lines - 1) * pieces

    def piece(i):
        up = lines - 1 - spot
        near = jnp.minimum(up, spot)
        lead = jnp.maximum(up, spot) - near
        sign = jnp.where(up >= spot, 1, -1)
        rest = jnp.maximum(i - lead * pieces, 0)
        turn = lax.rem(rest, 2 * pieces)
        side = jnp.where(lax.rem(turn, 2) == 0, -sign, sign)
        single = i < lead * pieces
        a = jnp.where(
            single,
            spot + sign * (lead + near - i // pieces),
            spot + side * (near - rest // (2 * pieces)),
        )
        p = jnp.where(single, lax.rem(i, pieces), turn // 2)
        own = i >= away
        return jnp.where(own, spot, a), jnp.where(own, i - away, p)

    def unpaired(sender, a, p):
        beside = (a == sender + 1) | (a == sender - 1)
        inner = (a == 0) | (a == lines - 1)
        outer = ((sender == 0) | (sender == lines - 1)) & (p < SKIP)
        return beside & (inner | outer)

    def cut_of(p):
        return pl.ds(pl.multiple_of(p * width, LANES), width)

    def core_copy(block, p, b):
        cut = cut_of(p)
        at = pl.ds(block * half, half)
        return pltpu.make_async_remote_copy(
            src_ref=image.at[at, b, 1 - core, :, :, cut], dst_ref=core_in.at[at, b, :, :, cut],
            send_sem=core_s.at[block, p, b], recv_sem=core_r.at[block, p, b],
            device_id={"freq": core_peer}, device_id_type=MESH,
        )

    def pair_copy(a, p):
        cut = cut_of(p)
        return pltpu.make_async_remote_copy(
            src_ref=image.at[a, 1 - pair, core, :, :, cut], dst_ref=pair_in.at[a, :, :, cut],
            send_sem=pair_s.at[a, p], recv_sem=pair_r.at[a, p],
            device_id={"freq": pair_peer}, device_id_type=MESH,
        )

    def low_copy(a, p):
        cut = cut_of(p)
        return pltpu.make_async_remote_copy(
            src_ref=image.at[a, pair, core, :, :, cut], dst_ref=low_in.at[a, :, :, cut],
            send_sem=low_s.at[a, p], recv_sem=low_r.at[a, p],
            device_id={"freq": jnp.minimum(spot + 1, lines - 1) * 4 + pair * 2 + core},
            device_id_type=MESH,
        )

    def high_copy(a, p):
        cut = cut_of(p)
        return pltpu.make_async_remote_copy(
            src_ref=image.at[a, pair, core, :, :, cut], dst_ref=high_in.at[a, :, :, cut],
            send_sem=high_s.at[a, p], recv_sem=high_r.at[a, p],
            device_id={"freq": jnp.maximum(spot - 1, 0) * 4 + pair * 2 + core},
            device_id_type=MESH,
        )

    def other_copy(upward, p):
        cut = cut_of(p)
        step = 1 if upward else -1
        return pltpu.make_async_remote_copy(
            src_ref=image.at[jnp.clip(spot + step, 0, lines - 1), 1 - pair, core, :, :, cut],
            dst_ref=other_in.at[0 if upward else 1, :, :, cut],
            send_sem=other_s.at[0 if upward else 1, p], recv_sem=other_r.at[0 if upward else 1, p],
            device_id={"freq": jnp.clip(spot + step, 0, lines - 1) * 4 + pair * 2 + core},
            device_id_type=MESH,
        )

    def block_of(c):
        if half == 1:
            return piece(c)
        return ranked(c // pieces, blocks, spot // half), lax.rem(c, pieces)

    def take_core(c):
        block, p = block_of(c)
        at = pl.ds(block * half, half)
        cut = cut_of(p)
        with scope("cw1"):
            core_copy(block, p, 1 - pair).wait_recv()
        image[at, 1 - pair, core, :, :, cut] = (
            image[at, 1 - pair, core, :, :, cut] + core_in[at, 1 - pair, :, :, cut]
        )
        for h in range(half):
            a = block * half + h
            skipped = unpaired(spot, a, p)

            @pl.when(jnp.logical_not(skipped) & (a != spot))
            def _():
                pair_copy(a, p).start()

            @pl.when(skipped & (a > spot))
            def _():
                other_copy(True, p).start()

            @pl.when(skipped & (a < spot))
            def _():
                other_copy(False, p).start()

        with scope("cw2"):
            core_copy(block, p, pair).wait_recv()
        image[at, pair, core, :, :, cut] = image[at, pair, core, :, :, cut] + core_in[at, pair, :, :, cut]

    def own_start(p):
        cut = cut_of(p)

        @pl.when((spot > 0) & unpaired(spot - 1, spot, p))
        def _():
            with scope("ow"):
                other_copy(True, p).wait_recv()
            image[spot, 1 - pair, core, :, :, cut] = image[spot, 1 - pair, core, :, :, cut] + other_in[0, :, :, cut]

        @pl.when((spot < lines - 1) & unpaired(spot + 1, spot, p))
        def _():
            with scope("ow"):
                other_copy(False, p).wait_recv()
            image[spot, 1 - pair, core, :, :, cut] = image[spot, 1 - pair, core, :, :, cut] + other_in[1, :, :, cut]

        pair_copy(spot, p).start()

    lag = LAG * jnp.minimum(spot, lines - 1 - spot)

    def step(i, carry):
        a, p = piece(jnp.minimum(i, away - 1))

        @pl.when((i < away) & jnp.logical_not(unpaired(spot, a, p)))
        def _():
            cut = cut_of(p)
            with scope("yw"):
                pair_copy(a, p).wait_recv()
            image[a, pair, core, :, :, cut] = image[a, pair, core, :, :, cut] + pair_in[a, :, :, cut]

        @pl.when(i >= lag)
        def _():
            a, p = piece(jnp.clip(i - lag, 0, away - 1))
            cut = cut_of(p)

            @pl.when(a > spot)
            def _():
                @pl.when(spot > 0)
                def _():
                    with scope("zw"):
                        low_copy(a, p).wait_recv()
                    image[a, pair, core, :, :, cut] = image[a, pair, core, :, :, cut] + low_in[a, :, :, cut]

                low_copy(a, p).start()

            @pl.when(a < spot)
            def _():
                @pl.when(spot < lines - 1)
                def _():
                    with scope("zw"):
                        high_copy(a, p).wait_recv()
                    image[a, pair, core, :, :, cut] = image[a, pair, core, :, :, cut] + high_in[a, :, :, cut]

                high_copy(a, p).start()

        @pl.when((i >= OWN) & (i < OWN + pieces))
        def _():
            own_start(i - OWN)

        return carry

    chunks = blocks * pieces

    def compute(c, carry):
        block, p = block_of(c)
        at = cut_of(p)

        @pl.when((c > 0) & (c < pieces))
        def _():
            x_table(p)

        with scope("dot"):
            lhs = field[p, pl.ds(2 * half * block, 2 * half)].reshape(half * 2 * radix * 16, 2 * width)
            res = jnp.dot(lhs, xtab[p], preferred_element_type=jnp.float32)
            res = res.reshape(half, 2, radix, 2, 8, width)
            for c_ in range(2):
                image[pl.ds(half * block, half), :, c_, :, :, at] = res[:, :, :, c_]
        core_copy(block, p, 1 - pair).start()
        core_copy(block, p, pair).start()

        @pl.when(c >= BEHIND)
        def _():
            take_core(c - BEHIND)

        return carry

    with scope("compute"):
        lax.fori_loop(0, chunks, compute, 0)
        lax.fori_loop(chunks - BEHIND, chunks, lambda c, carry: (take_core(c), carry)[1], 0)

    with scope("third"):
        lax.fori_loop(0, away + lag, step, 0)

    def energy_take(i, total):
        energy_copy(i).wait_recv()
        return total + eall[i]

    total = lax.fori_loop(1, groups, energy_take, etile[...])
    total = jnp.sum(jnp.sum(total, axis=0, keepdims=True), axis=1, keepdims=True)
    scale = lax.rsqrt(total / freq_total + 1e-06)

    lanes8 = lax.broadcasted_iota(jnp.int32, (8, LANES), 1)
    part_lane = lanes8 // pieces
    lane_part = lax.rem(lanes8, pieces)

    def own(p, carry):
        cut = cut_of(p)
        with scope("oyw"):
            pair_copy(spot, p).wait_recv()
        image[spot, pair, core, :, :, cut] = image[spot, pair, core, :, :, cut] + pair_in[spot, :, :, cut]

        @pl.when(spot > 0)
        def _():
            with scope("ozw"):
                low_copy(spot, p).wait_recv()
            image[spot, pair, core, :, :, cut] = image[spot, pair, core, :, :, cut] + low_in[spot, :, :, cut]

        @pl.when(spot < lines - 1)
        def _():
            with scope("ozw"):
                high_copy(spot, p).wait_recv()
            image[spot, pair, core, :, :, cut] = image[spot, pair, core, :, :, cut] + high_in[spot, :, :, cut]

        for n1 in range(radix):
            for j in range(tiles):
                source = pl.ds(pl.multiple_of(p * width + j // pieces * LANES, LANES), LANES)
                value = image[spot, pair, core, n1, :, source] * scale
                spread = jnp.take_along_axis(value, part_lane + j % pieces * (LANES // pieces), axis=1)
                to = slice(j * LANES, (j + 1) * LANES)
                out_ref[:, n1, to] = jnp.where(lane_part == p, spread, out_ref[:, n1, to])
        return carry

    with scope("own"):
        lax.fori_loop(0, pieces, own, 0)

    def energy_end(i, carry):
        energy_copy(i).wait_send()
        return carry

    lax.fori_loop(1, groups, energy_end, 0)

    def finish_core(block, carry):
        def ended(p, inner):
            core_copy(block, p, 0).wait_send()
            core_copy(block, p, 1).wait_send()
            return inner

        return lax.fori_loop(0, pieces, ended, carry)

    lax.fori_loop(0, blocks, finish_core, 0)

    def finish(a, carry):
        def ended(p, inner):
            @pl.when(jnp.logical_not(unpaired(spot, a, p)))
            def _():
                pair_copy(a, p).wait_send()

            @pl.when(unpaired(spot, a, p) & (a > spot))
            def _():
                other_copy(True, p).wait_send()

            @pl.when(unpaired(spot, a, p) & (a < spot))
            def _():
                other_copy(False, p).wait_send()

            @pl.when(a > spot)
            def _():
                low_copy(a, p).wait_send()

            @pl.when(a < spot)
            def _():
                high_copy(a, p).wait_send()

            return inner

        return lax.fori_loop(0, pieces, ended, carry)

    lax.fori_loop(0, lines, finish, 0)


def body(spectra, wavelet, freq_index, slowness, layer_ids, ray_slowness):
    slot_total, unused, rows, cols = spectra.shape
    groups = lax.axis_size("freq")
    freq_total = slot_total * groups
    radix = rows // groups // 8
    short = rows // radix
    lines = groups // 4
    pieces = min(4, cols // LANES)
    f32, bf16 = jnp.float32, jnp.bfloat16
    dma = pltpu.SemaphoreType.DMA
    out = pl.pallas_call(
        functools.partial(kernel, groups, radix, pieces, freq_total),
        out_shape=jax.ShapeDtypeStruct((8, radix, cols), f32),
        in_specs=[
            *[pl.BlockSpec(memory_space=pltpu.SMEM)] * 5,
            pl.BlockSpec(memory_space=pl.ANY),
        ],
        out_specs=pl.BlockSpec(memory_space=pltpu.VMEM),
        scratch_shapes=[
            pltpu.VMEM((2, radix, short, cols), bf16),
            pltpu.VMEM((radix, 2 * short, cols), bf16),
            pltpu.VMEM((radix, 2 * short, 2 * short), bf16),
            pltpu.VMEM((pieces, groups // 2, radix, 16, 2 * (cols // pieces)), bf16),
            pltpu.VMEM((pieces, 2 * (cols // pieces), cols // pieces), bf16),
            pltpu.VMEM((pieces, 2 * short, cols // pieces), f32),
            pltpu.VMEM((2, rows, cols), f32),
            pltpu.VMEM((lines, 2, 2, radix, 8, cols), f32),
            pltpu.VMEM((lines, 2, radix, 8, cols), f32),
            pltpu.VMEM((lines, radix, 8, cols), f32),
            pltpu.VMEM((lines, radix, 8, cols), f32),
            pltpu.VMEM((lines, radix, 8, cols), f32),
            pltpu.VMEM((2, radix, 8, cols), f32),
            pltpu.VMEM((8, LANES), f32),
            pltpu.VMEM((groups, 8, LANES), f32),
            dma((short // 16,)),
            dma((min(lines, 4), pieces, 2)),
            dma((min(lines, 4), pieces, 2)),
            dma((lines, pieces)),
            dma((lines, pieces)),
            dma((lines, pieces)),
            dma((lines, pieces)),
            dma((lines, pieces)),
            dma((lines, pieces)),
            dma((2, pieces)),
            dma((2, pieces)),
            dma((groups,)),
            dma((groups,)),
        ],
        compiler_params=pltpu.CompilerParams(
            collective_id=0, has_side_effects=True, vmem_limit_bytes=60 * 1024 * 1024
        ),
    )(
        wavelet, freq_index.reshape(1, 1), slowness, layer_ids.reshape(1, 1), ray_slowness,
        spectra.reshape(2, radix, short, cols),
    )
    return out.reshape(1, 8 * radix, cols)


def solution(mesh):
    placed = (
        P(("rays", "freq"), None, None, None),
        P("freq", None),
        P("freq"),
        P(),
        P(),
        P("rays"),
    )
    return jax.shard_map(
        body, mesh=mesh, in_specs=placed, out_specs=P("rays", "freq", None), check_vma=False
    )
```

```python
import contextlib
import functools
import math

import jax
import jax.numpy as jnp
from jax import lax
from jax.experimental import pallas as pl
from jax.experimental.pallas import tpu as pltpu
from jax.sharding import PartitionSpec as P

GRID_STEP = 12.5
DEPTH_STEP = 10.0
LOW_FREQUENCY = 5.0
FREQUENCY_BAND = 50.0
DAMPING = 6.0
LANES = 128
LAG = 2
BEHIND = 3
SKIP = 2
FIRST = 2
HEAD = 1
EARLY = (11, 14)
OWN = 4
YTALL = 64
MESH = pl.DeviceIdType.MESH

HALF_SIN = (0.9999998807907104, -0.16666465997695923, 0.008326363749802113, -0.00019062065985053778)
HALF_COS = (0.9999992251396179, -0.499982088804245, 0.04160428047180176, -0.0013190462486818433)
TURN_SIN = (0.9999992251396179, -0.16665679216384888, 0.008313224650919437, -0.0001852344867074862)
TURN_COS = (
    0.9999999403953552, -0.4999990463256836, 0.041663579642772675, -0.0013853666605427861,
    2.315317397005856e-05,
)

ROOT = math.sqrt(2.0)
PHASE_SIN = tuple(ROOT * c / 2.0 ** (2 * k + 1) for k, c in enumerate(HALF_SIN))
PHASE_COS = tuple(ROOT * c / 4.0**k for k, c in enumerate(HALF_COS))


def scope(name):
    return contextlib.nullcontext()


def polynomial(coefs, square):
    value = square * coefs[-1] + coefs[-2]
    for coef in coefs[-3::-1]:
        value = value * square + coef
    return value


def half_sincos(half, sin_coefs, cos_coefs):
    square = half * half
    sine = polynomial(sin_coefs, square) * half
    twice = sine + sine
    return twice * polynomial(cos_coefs, square), 1.0 - twice * sine


def turn_sincos(turns):
    reduced = turns - jnp.floor(turns + 0.5)
    return half_sincos(reduced * math.pi, TURN_SIN, TURN_COS)


def butterfly(parts):
    count = len(parts)
    if count == 1:
        return parts
    even = butterfly(parts[0::2])
    odd = butterfly(parts[1::2])
    low, high = [], []
    for i in range(count // 2):
        er, ei = even[i]
        xr, xi = odd[i]
        if i == 0:
            tr, ti = xr, xi
        elif 4 * i == count:
            tr, ti = -xi, xr
        elif 8 * i == count:
            root = math.sqrt(0.5)
            tr, ti = (xr - xi) * root, (xr + xi) * root
        elif 8 * i == 3 * count:
            root = math.sqrt(0.5)
            tr, ti = (xr + xi) * -root, (xr - xi) * root
        else:
            c = math.cos(2 * math.pi * i / count)
            s = math.sin(2 * math.pi * i / count)
            tr, ti = xr * c - xi * s, xr * s + xi * c
        low.append((er + tr, ei + ti))
        high.append((er - tr, ei - ti))
    return low + high


def kernel(
    groups, radix, pieces, freq_total,
    wavelet, freq_index, slowness, layer_ids, rays, spec_hbm, out_ref,
    spec, zed, ytab, field, xtab, yout, fac, image, core_in, pair_in, low_in, high_in, other_in, etile, eall,
    load_sem, core_s, core_r, pair_s, pair_r, line_s, line_r, other_r, e_s, e_r,
):
    rows = spec.shape[1] * spec.shape[2]
    cols = spec.shape[3]
    short = rows // radix
    lines = groups // 4
    me = lax.axis_index("freq")
    core = lax.rem(me, 2)
    pair = lax.rem(me // 2, 2)
    spot = me // 4
    core_peer = me + 1 - 2 * core
    pair_peer = me + 2 - 4 * pair

    barrier = pltpu.get_barrier_semaphore()

    with scope("begin"):
        core_peer = core_peer + 0

    def greet(i, carry):
        pl.semaphore_signal(
            barrier, inc=1, device_id={"freq": lax.rem(me + i, groups)}, device_id_type=MESH
        )
        return carry

    with scope("greet"):
        lax.fori_loop(1, groups, greet, 0)

    strips = short // 16
    tiles = cols // LANES

    def load(i):
        window = pl.ds(pl.multiple_of(i * 16, 16), 16)
        return pltpu.make_async_copy(
            spec_hbm.at[:, :, window, :], spec.at[:, :, window, :], load_sem
        )

    def start_load(i, carry):
        load(i).start()
        return carry

    with scope("loads"):
        lax.fori_loop(0, strips, start_load, 0)

    hertz = freq_index[0, 0].astype(jnp.float32) * (FREQUENCY_BAND / freq_total) + LOW_FREQUENCY
    angular = hertz * (2.0 * math.pi)
    slow = slowness[layer_ids[0, 0]]
    slow_sq = slow * slow
    ray_x = rays[0]
    ray_y = rays[1]
    real_base = (angular * angular - DAMPING * DAMPING) * slow_sq
    imag_arg = 2.0 * angular * DAMPING * slow_sq
    turn_x = hertz * ray_x * GRID_STEP
    turn_y = hertz * ray_y * GRID_STEP
    vertical = jnp.full((YTALL, LANES), slow_sq - ray_x * ray_x - ray_y * ray_y, jnp.float32)
    turn_0 = jnp.sqrt(vertical) * (DEPTH_STEP * hertz)
    wave_re = wavelet[0, 0]
    wave_im = wavelet[0, 1]

    width = cols // pieces
    deep = 32

    def x_table(p):
        x = lax.broadcasted_iota(jnp.int32, (deep, width), 1) * pieces + p
        x = x.astype(jnp.float32)
        away = x * turn_x
        away = away - jnp.floor(away)
        x = x * (1.0 / cols)
        k = lax.broadcasted_iota(jnp.int32, (deep, width), 0)

        def strip_of(strip, carry):
            sine, cosine = turn_sincos((k + strip * deep).astype(jnp.float32) * x + away)
            row = pl.ds(pl.multiple_of(strip * deep, deep), deep)
            row_im = pl.ds(pl.multiple_of(strip * deep + width, deep), deep)
            xtab[p, row, :] = cosine.astype(jnp.bfloat16)
            xtab[p, row_im, :] = (-sine).astype(jnp.bfloat16)
            return carry

        lax.fori_loop(0, width // deep, strip_of, 0, unroll=True)

    with scope("xt0"):
        x_table(0)

    ytiles = short // LANES

    tall = short // YTALL

    def y_table(step, carry):
        n1 = step // (tall * ytiles)
        strip = lax.rem(step // ytiles, tall)
        tile = lax.rem(step, ytiles)
        n2 = lax.broadcasted_iota(jnp.int32, (YTALL, LANES), 0) + strip * YTALL
        k2 = lax.broadcasted_iota(jnp.int32, (YTALL, LANES), 1) + tile * LANES
        n = n2 * radix + n1
        n = n.astype(jnp.float32)
        turns = k2.astype(jnp.float32) * (n * (1.0 / rows))
        turns = turns - jnp.floor(turns)
        sine, cosine = turn_sincos(turns + n * turn_y + turn_0)
        real = (wave_re * cosine + wave_im * sine).astype(jnp.bfloat16)
        imag_f = wave_re * sine - wave_im * cosine
        imag = imag_f.astype(jnp.bfloat16)
        top = pl.ds(pl.multiple_of(strip * YTALL, YTALL), YTALL)
        bottom = pl.ds(pl.multiple_of(strip * YTALL + short, YTALL), YTALL)
        left = pl.ds(pl.multiple_of(tile * LANES, LANES), LANES)
        right = pl.ds(pl.multiple_of(tile * LANES + short, LANES), LANES)
        ytab[n1, top, left] = real
        ytab[n1, top, right] = (-imag_f).astype(jnp.bfloat16)
        ytab[n1, bottom, left] = imag
        ytab[n1, bottom, right] = real
        return carry

    with scope("ytab"):
        lax.fori_loop(0, radix * tall * ytiles, y_table, 0, unroll=2)

    half_gain = 0.5 * DEPTH_STEP * DEPTH_STEP
    step_y = 2.0 * math.pi / (rows * GRID_STEP) * math.sqrt(half_gain)
    step_x = 2.0 * math.pi / (cols * GRID_STEP) * math.sqrt(half_gain)
    base = real_base * half_gain
    imag = imag_arg * half_gain
    imag_sq = imag * imag

    def factor(a):
        m = a * a + imag_sq
        q = m * lax.rsqrt(m) + jnp.abs(a)
        iq = lax.rsqrt(q)
        g = q * iq
        h = imag * iq
        forward = a >= 0.0
        vert_re = jnp.where(forward, g, h)
        vert_im = jnp.where(forward, h, g)
        damp = jnp.exp2(vert_im * -math.log2(math.e))
        square = vert_re * vert_re
        v = polynomial(PHASE_SIN, square) * vert_re
        w = polynomial(PHASE_COS, square)
        dv = damp * v
        return damp - dv * v, dv * w

    def signed(index, extent):
        return jnp.where(index >= extent // 2, index - extent, index).astype(jnp.float32)

    lane = lax.broadcasted_iota(jnp.int32, (8, LANES), 1)
    sub = lax.broadcasted_iota(jnp.int32, (8, LANES), 0)
    kx_sq = []
    for t in range(tiles // 2):
        kx = (lane + t * LANES).astype(jnp.float32) * step_x
        kx_sq.append(kx * kx)
    edge_x = cols // 2 * step_x
    turned = lax.rem(LANES - lane, LANES)
    flipped = lax.rem(8 - sub, 8)
    first = lane == 0
    top = sub == 0
    edge_y = (lane * 8 + sub).astype(jnp.float32) * step_y
    edge = factor(base - edge_x * edge_x - edge_y * edge_y)

    def factor_rows(m, put):
        ky = (sub + m * 8).astype(jnp.float32) * step_y
        ybase = base - ky * ky
        here = jnp.full((8, LANES), m, jnp.int32)
        after = [jnp.take_along_axis(e, here, axis=1) for e in edge]
        for t in reversed(range(tiles // 2)):
            now = factor(ybase - kx_sq[t])
            for c in range(2):
                put(c, t, now[c])
                back = jnp.take_along_axis(now[c], turned, axis=1)
                put(c, tiles - 1 - t, jnp.where(first, after[c], back))
            after = now

    middle = {}

    def put_middle(c, t, value):
        middle[c, t] = value

    def factors(i, carry):
        m = rows // 16 - 1 - i
        here = pl.ds(pl.multiple_of(m * 8, 8), 8)
        values = {}
        low = pl.ds(pl.multiple_of(rows - 8 - m * 8, 8), 8)

        def put(c, t, value):
            at = slice(t * LANES, (t + 1) * LANES)
            fac[c, low, at] = jnp.where(top, carry[c, t], jnp.take_along_axis(value, flipped, axis=0))
            fac[c, here, at] = value
            values[c, t] = value

        factor_rows(m, put)
        return values

    with scope("factors"):
        factor_rows(rows // 16, put_middle)
        lax.fori_loop(0, rows // 16, factors, middle, unroll=8)

    def shift(strip, total):
        rows_at = pl.ds(pl.multiple_of(strip * 16, 16), 16)

        def inner(tile, acc):
            at = pl.ds(pl.multiple_of(tile * LANES, LANES), LANES)
            parts = []
            for k1 in range(radix):
                row = pl.ds(pl.multiple_of(strip * 16 + k1 * short, 16), 16)
                cosine = fac[0, row, at]
                sine = fac[1, row, at]
                re = spec[0, k1, rows_at, at].astype(jnp.float32)
                im = spec[1, k1, rows_at, at].astype(jnp.float32)
                new_re = re * cosine - im * sine
                new_im = re * sine + im * cosine
                acc = acc + (new_re * new_re + new_im * new_im)
                parts.append((new_re.astype(jnp.bfloat16), new_im.astype(jnp.bfloat16)))
            for n1, (re, im) in enumerate(butterfly(parts)):
                zed[n1, rows_at, at] = re
                low = pl.ds(pl.multiple_of(strip * 16 + short, 16), 16)
                zed[n1, low, at] = im
            return acc

        return lax.fori_loop(0, tiles, inner, total, unroll=8)

    with scope("shift"):
        pltpu.make_async_copy(spec_hbm, spec, load_sem).wait()
        energy = lax.fori_loop(0, strips, shift, jnp.zeros((16, LANES), jnp.float32))
    etile[...] = energy[:8] + energy[8:]

    chips = groups // 2

    def y_stage(n1, carry):
        for part in range(pieces):
            at = slice(part * width, (part + 1) * width)
            yout[part] = jnp.dot(ytab[n1], zed[n1, :, at], preferred_element_type=jnp.float32)

        def fold(strip, inner):
            top = pl.ds(pl.multiple_of(strip * 16, 16), 16)
            low = pl.ds(pl.multiple_of(strip * 16 + short, 16), 16)
            for lane_tile in range(width // LANES):
                left = slice(lane_tile * LANES, (lane_tile + 1) * LANES)
                right = slice(width + lane_tile * LANES, width + (lane_tile + 1) * LANES)
                terms = [(yout[part, top, left], yout[part, low, left]) for part in range(pieces)]
                for x1, (re, im) in enumerate(butterfly(terms)):
                    field[x1, strip, n1, :, left] = re.astype(jnp.bfloat16)
                    field[x1, strip, n1, :, right] = im.astype(jnp.bfloat16)
            return inner

        lax.fori_loop(0, chips, fold, 0, unroll=True)
        return carry

    with scope("ystage"):
        lax.fori_loop(0, radix, y_stage, 0, unroll=True)

    with scope("barr"):
        pl.semaphore_wait(barrier, groups - 1)

    def energy_copy(i):
        return pltpu.make_async_remote_copy(
            src_ref=etile, dst_ref=eall.at[i], send_sem=e_s, recv_sem=e_r,
            device_id={"freq": lax.rem(me + i, groups)}, device_id_type=MESH,
        )

    def energy_start(i, carry):
        energy_copy(i).start()
        return carry

    lax.fori_loop(1, groups, energy_start, 0)

    def ranked(j, count, centre):
        up = count - 1 - centre
        near = jnp.minimum(up, centre)
        lead = jnp.maximum(up, centre) - near
        sign = jnp.where(up >= centre, 1, -1)
        rest = jnp.maximum(j - lead, 0)
        side = jnp.where(lax.rem(rest, 2) == 0, sign, -sign)
        return jnp.where(j < lead, centre + sign * (lead + near - j), centre + side * (near - rest // 2))

    half = max(lines // 4, 1)
    blocks = lines // half
    away = (lines - 1) * pieces

    def piece(i):
        up = lines - 1 - spot
        near = jnp.minimum(up, spot)
        lead = jnp.maximum(up, spot) - near
        sign = jnp.where(up >= spot, 1, -1)
        rest = jnp.maximum(i - lead * pieces, 0)
        turn = lax.rem(rest, 2 * pieces)
        side = jnp.where(lax.rem(turn, 2) == 0, -sign, sign)
        single = i < lead * pieces
        a = jnp.where(
            single,
            spot + sign * (lead + near - i // pieces),
            spot + side * (near - rest // (2 * pieces)),
        )
        p = jnp.where(single, lax.rem(i, pieces), turn // 2)
        own = i >= away
        return jnp.where(own, spot, a), jnp.where(own, i - away, p)

    def unpaired(sender, a, p):
        beside = (a == sender + 1) | (a == sender - 1)
        inner = (a == 0) | (a == lines - 1)
        outer = ((sender == 0) | (sender == lines - 1)) & (p < SKIP)
        return beside & (inner | outer)

    def cut_of(p):
        return pl.ds(pl.multiple_of(p * width, LANES), width)

    def core_copy(block, p):
        cut = cut_of(p)
        at = pl.ds(block * half, half)
        return pltpu.make_async_remote_copy(
            src_ref=image.at[at, :, 1 - core, :, :, cut], dst_ref=core_in.at[at, :, :, :, cut],
            send_sem=core_s, recv_sem=core_r.at[block, p],
            device_id={"freq": core_peer}, device_id_type=MESH,
        )

    def pair_copy(a, p):
        cut = cut_of(p)
        return pltpu.make_async_remote_copy(
            src_ref=image.at[a, 1 - pair, core, :, :, cut], dst_ref=pair_in.at[a, :, :, cut],
            send_sem=pair_s, recv_sem=pair_r.at[a, p],
            device_id={"freq": pair_peer}, device_id_type=MESH,
        )

    def low_copy(a, p):
        cut = cut_of(p)
        return pltpu.make_async_remote_copy(
            src_ref=image.at[a, pair, core, :, :, cut], dst_ref=low_in.at[a, :, :, cut],
            send_sem=line_s, recv_sem=line_r.at[a, p],
            device_id={"freq": jnp.minimum(spot + 1, lines - 1) * 4 + pair * 2 + core},
            device_id_type=MESH,
        )

    def high_copy(a, p, arriving=False):
        cut = cut_of(p)
        return pltpu.make_async_remote_copy(
            src_ref=image.at[a, pair, core, :, :, cut], dst_ref=high_in.at[a, :, :, cut],
            send_sem=line_s, recv_sem=line_r.at[jnp.where(a == (spot if arriving else spot - 1), lines, a), p],
            device_id={"freq": jnp.maximum(spot - 1, 0) * 4 + pair * 2 + core},
            device_id_type=MESH,
        )

    def other_copy(upward, p):
        cut = cut_of(p)
        step = 1 if upward else -1
        return pltpu.make_async_remote_copy(
            src_ref=image.at[jnp.clip(spot + step, 0, lines - 1), 1 - pair, core, :, :, cut],
            dst_ref=other_in.at[0 if upward else 1, :, :, cut],
            send_sem=pair_s, recv_sem=other_r.at[0 if upward else 1, p],
            device_id={"freq": jnp.clip(spot + step, 0, lines - 1) * 4 + pair * 2 + core},
            device_id_type=MESH,
        )

    ends = (spot == 0) | (spot == lines - 1)

    def block_of(c):
        if half == 1:
            near = (lines - 2) * pieces
            moved = jnp.where(c < FIRST + SKIP, near + c - FIRST, c - SKIP)
            return piece(jnp.where(ends & (c >= FIRST) & (c < near + SKIP), moved, c))
        return ranked(c // pieces, blocks, spot // half), lax.rem(c, pieces)

    def hasty(a, p):
        return unpaired(spot, a, p) & (p < HEAD)

    def take_core(c):
        block, p = block_of(c)
        at = pl.ds(block * half, half)
        cut = cut_of(p)
        with scope("cw1"):
            core_copy(block, p).wait_recv()
        image[at, 1 - pair, core, :, :, cut] = (
            image[at, 1 - pair, core, :, :, cut] + core_in[at, 1 - pair, :, :, cut]
        )
        for h in range(half):
            a = block * half + h
            skipped = unpaired(spot, a, p)

            @pl.when(jnp.logical_not(skipped) & (a != spot))
            def _():
                pair_copy(a, p).start()

            @pl.when(skipped & (a > spot))
            def _():
                other_copy(True, p).start()

            @pl.when(skipped & (a < spot))
            def _():
                other_copy(False, p).start()

        image[at, pair, core, :, :, cut] = image[at, pair, core, :, :, cut] + core_in[at, pair, :, :, cut]
        for h in range(half):
            a = block * half + h

            @pl.when((spot == 0) & hasty(a, p))
            def _():
                low_copy(a, p).start()

            @pl.when((spot == lines - 1) & hasty(a, p))
            def _():
                high_copy(a, p).start()

    def own_start(p):
        cut = cut_of(p)

        @pl.when((spot > 0) & unpaired(spot - 1, spot, p))
        def _():
            with scope("ow"):
                other_copy(True, p).wait_recv()
            image[spot, 1 - pair, core, :, :, cut] = image[spot, 1 - pair, core, :, :, cut] + other_in[0, :, :, cut]

        @pl.when((spot < lines - 1) & unpaired(spot + 1, spot, p))
        def _():
            with scope("ow"):
                other_copy(False, p).wait_recv()
            image[spot, 1 - pair, core, :, :, cut] = image[spot, 1 - pair, core, :, :, cut] + other_in[1, :, :, cut]

        pair_copy(spot, p).start()

    lag = LAG * jnp.minimum(spot, lines - 1 - spot)

    def step(i, carry):
        a, p = piece(jnp.minimum(i, away - 1))

        @pl.when((i < away) & jnp.logical_not(unpaired(spot, a, p)))
        def _():
            cut = cut_of(p)
            with scope("yw"):
                pair_copy(a, p).wait_recv()
            image[a, pair, core, :, :, cut] = image[a, pair, core, :, :, cut] + pair_in[a, :, :, cut]

        @pl.when(i >= lag)
        def _():
            a, p = piece(jnp.clip(i - lag, 0, away - 1))
            cut = cut_of(p)

            @pl.when((a > spot) & jnp.logical_not((spot == 0) & hasty(a, p)))
            def _():
                @pl.when(spot > 0)
                def _():
                    with scope("zw"):
                        low_copy(a, p).wait_recv()
                    image[a, pair, core, :, :, cut] = image[a, pair, core, :, :, cut] + low_in[a, :, :, cut]

                low_copy(a, p).start()

            @pl.when((a < spot) & jnp.logical_not((spot == lines - 1) & hasty(a, p)))
            def _():
                @pl.when(spot < lines - 1)
                def _():
                    with scope("zw"):
                        high_copy(a, p, True).wait_recv()
                    image[a, pair, core, :, :, cut] = image[a, pair, core, :, :, cut] + high_in[a, :, :, cut]

                high_copy(a, p).start()

        @pl.when((i >= OWN) & (i < OWN + pieces))
        def _():
            own_start(i - OWN)

        return carry

    chunks = blocks * pieces

    def compute(c, carry):
        block, p = block_of(c)
        at = cut_of(p)

        with scope("dot"):
            lhs = field[p, pl.ds(2 * half * block, 2 * half)].reshape(half * 2 * radix * 16, 2 * width)
            res = jnp.dot(lhs, xtab[p], preferred_element_type=jnp.float32)
            res = res.reshape(half, 2, radix, 2, 8, width)
            for c_ in range(2):
                image[pl.ds(half * block, half), :, c_, :, :, at] = res[:, :, :, c_]
        core_copy(block, p).start()

        @pl.when(c == 0)
        def _():
            with scope("xt"):
                lax.fori_loop(1, pieces, lambda p, carry: (x_table(p), carry)[1], 0)
            take_core(c)

        @pl.when(c > BEHIND)
        def _():
            take_core(c - BEHIND)

        for i, at_chunk in enumerate(EARLY):
            @pl.when(c == min(at_chunk, chunks - 1))
            def _():
                step(i, 0)

        return carry

    with scope("compute"):
        lax.fori_loop(0, chunks, compute, 0)
        lax.fori_loop(chunks - BEHIND, chunks, lambda c, carry: (take_core(c), carry)[1], 0)

    with scope("third"):
        lax.fori_loop(len(EARLY), away + lag, step, 0)

    def all_sent(sem, ref):
        pltpu.make_async_remote_copy(
            src_ref=ref, dst_ref=ref, send_sem=sem, recv_sem=sem,
            device_id={"freq": core_peer}, device_id_type=MESH,
        ).wait_send()

    all_sent(e_r, eall.at[1:groups])

    def energy_take(i, total):
        return total + eall[i]

    total = lax.fori_loop(1, groups, energy_take, etile[...])
    total = jnp.sum(jnp.sum(total, axis=0, keepdims=True), axis=1, keepdims=True)
    scale = lax.rsqrt(total / freq_total + 1e-06)

    all_sent(e_s, eall.at[1:groups])
    all_sent(core_s, core_in)

    lanes8 = lax.broadcasted_iota(jnp.int32, (8, LANES), 1)
    part_lane = lanes8 // pieces
    lane_part = lax.rem(lanes8, pieces)

    def own(p, carry):
        cut = cut_of(p)
        with scope("oyw"):
            pair_copy(spot, p).wait_recv()
        image[spot, pair, core, :, :, cut] = image[spot, pair, core, :, :, cut] + pair_in[spot, :, :, cut]

        @pl.when(spot > 0)
        def _():
            with scope("ozw"):
                low_copy(spot, p).wait_recv()
            image[spot, pair, core, :, :, cut] = image[spot, pair, core, :, :, cut] + low_in[spot, :, :, cut]

        @pl.when(spot < lines - 1)
        def _():
            with scope("ozw"):
                high_copy(spot, p, True).wait_recv()
            image[spot, pair, core, :, :, cut] = image[spot, pair, core, :, :, cut] + high_in[spot, :, :, cut]

        for n1 in range(radix):
            for j in range(tiles):
                source = pl.ds(pl.multiple_of(p * width + j // pieces * LANES, LANES), LANES)
                value = image[spot, pair, core, n1, :, source] * scale
                spread = jnp.take_along_axis(value, part_lane + j % pieces * (LANES // pieces), axis=1)
                to = slice(j * LANES, (j + 1) * LANES)
                out_ref[:, n1, to] = jnp.where(lane_part == p, spread, out_ref[:, n1, to])
        return carry

    with scope("own"):
        lax.fori_loop(0, pieces, own, 0)

    with scope("ownend"):
        all_sent(line_s, pair_in.at[1:lines])
        all_sent(pair_s, pair_in)


def body(spectra, wavelet, freq_index, slowness, layer_ids, ray_slowness):
    slot_total, unused, rows, cols = spectra.shape
    groups = lax.axis_size("freq")
    freq_total = slot_total * groups
    radix = rows // groups // 8
    short = rows // radix
    lines = groups // 4
    pieces = min(4, cols // LANES)
    f32, bf16 = jnp.float32, jnp.bfloat16
    dma = pltpu.SemaphoreType.DMA
    out = pl.pallas_call(
        functools.partial(kernel, groups, radix, pieces, freq_total),
        out_shape=pltpu.VMEM((8, radix, cols), f32),
        in_specs=[
            *[pl.BlockSpec(memory_space=pltpu.SMEM)] * 5,
            pl.BlockSpec(memory_space=pl.ANY),
        ],
        out_specs=pl.BlockSpec(memory_space=pltpu.VMEM),
        scratch_shapes=[
            pltpu.VMEM((2, radix, short, cols), bf16),
            pltpu.VMEM((radix, 2 * short, cols), bf16),
            pltpu.VMEM((radix, 2 * short, 2 * short), bf16),
            pltpu.VMEM((pieces, groups // 2, radix, 16, 2 * (cols // pieces)), bf16),
            pltpu.VMEM((pieces, 2 * (cols // pieces), cols // pieces), bf16),
            pltpu.VMEM((pieces, 2 * short, cols // pieces), f32),
            pltpu.VMEM((2, rows, cols), f32),
            pltpu.VMEM((lines, 2, 2, radix, 8, cols), f32),
            pltpu.VMEM((lines, 2, radix, 8, cols), f32),
            pltpu.VMEM((lines, radix, 8, cols), f32),
            pltpu.VMEM((lines, radix, 8, cols), f32),
            pltpu.VMEM((lines, radix, 8, cols), f32),
            pltpu.VMEM((2, radix, 8, cols), f32),
            pltpu.VMEM((8, LANES), f32),
            pltpu.VMEM((groups, 8, LANES), f32),
            dma,
            dma,
            dma((min(lines, 4), pieces)),
            dma,
            dma((lines, pieces)),
            dma,
            dma((lines + 1, pieces)),
            dma((2, pieces)),
            dma,
            dma,
        ],
        compiler_params=pltpu.CompilerParams(
            collective_id=0, has_side_effects=True, vmem_limit_bytes=60 * 1024 * 1024
        ),
    )(
        wavelet, freq_index.reshape(1, 1), slowness, layer_ids.reshape(1, 1), ray_slowness,
        spectra.reshape(2, radix, short, cols),
    )
    return out.reshape(1, 8 * radix, cols)


def solution(mesh):
    placed = (
        P(("rays", "freq"), None, None, None),
        P("freq", None),
        P("freq"),
        P(),
        P(),
        P("rays"),
    )
    return jax.shard_map(
        body, mesh=mesh, in_specs=placed, out_specs=P("rays", "freq", None), check_vma=False
    )
```

```python
import contextlib
import functools
import math

import jax
import jax.numpy as jnp
from jax import lax
from jax.experimental import pallas as pl
from jax.experimental.pallas import tpu as pltpu
from jax.sharding import PartitionSpec as P

GRID_STEP = 12.5
DEPTH_STEP = 10.0
LOW_FREQUENCY = 5.0
FREQUENCY_BAND = 50.0
DAMPING = 6.0
LANES = 128
LAG = 2
BEHIND = 3
SKIP = 2
FIRST = 2
HEAD = 1
EARLY = (11, 14)
OWN = 4
YTALL = 64
MESH = pl.DeviceIdType.MESH

HALF_SIN = (0.9999998807907104, -0.16666465997695923, 0.008326363749802113, -0.00019062065985053778)
HALF_COS = (0.9999992251396179, -0.499982088804245, 0.04160428047180176, -0.0013190462486818433)
TURN_SIN = (0.9999992251396179, -0.16665679216384888, 0.008313224650919437, -0.0001852344867074862)
TURN_COS = (
    0.9999999403953552, -0.4999990463256836, 0.041663579642772675, -0.0013853666605427861,
    2.315317397005856e-05,
)

ROOT = math.sqrt(2.0)
PHASE_SIN = tuple(ROOT * c / 2.0 ** (2 * k + 1) for k, c in enumerate(HALF_SIN))
PHASE_COS = tuple(ROOT * c / 4.0**k for k, c in enumerate(HALF_COS))


def scope(name):
    return contextlib.nullcontext()


def polynomial(coefs, square):
    value = square * coefs[-1] + coefs[-2]
    for coef in coefs[-3::-1]:
        value = value * square + coef
    return value


def half_sincos(half, sin_coefs, cos_coefs):
    square = half * half
    sine = polynomial(sin_coefs, square) * half
    twice = sine + sine
    return twice * polynomial(cos_coefs, square), 1.0 - twice * sine


def turn_sincos(turns):
    reduced = turns - jnp.floor(turns + 0.5)
    return half_sincos(reduced * math.pi, TURN_SIN, TURN_COS)


def butterfly(parts):
    count = len(parts)
    if count == 1:
        return parts
    even = butterfly(parts[0::2])
    odd = butterfly(parts[1::2])
    low, high = [], []
    for i in range(count // 2):
        er, ei = even[i]
        xr, xi = odd[i]
        if i == 0:
            tr, ti = xr, xi
        elif 4 * i == count:
            tr, ti = -xi, xr
        elif 8 * i == count:
            root = math.sqrt(0.5)
            tr, ti = (xr - xi) * root, (xr + xi) * root
        elif 8 * i == 3 * count:
            root = math.sqrt(0.5)
            tr, ti = (xr + xi) * -root, (xr - xi) * root
        else:
            c = math.cos(2 * math.pi * i / count)
            s = math.sin(2 * math.pi * i / count)
            tr, ti = xr * c - xi * s, xr * s + xi * c
        low.append((er + tr, ei + ti))
        high.append((er - tr, ei - ti))
    return low + high


def kernel(
    groups, radix, pieces, freq_total,
    wavelet_hbm, freq_hbm, slowness_hbm, layer_hbm, rays_hbm, spec_hbm, out_ref,
    wavelet, freq_index, slowness, layer_ids, rays,
    spec, zed, ytab, field, xtab, yout, vecs, xbase, fac, mixed, image, core_in, pair_in, low_in, high_in, other_in, etile, eall,
    small_sem, load_sem, core_s, core_r, pair_s, pair_r, line_s, line_r, other_r, e_s, e_r,
):
    rows = spec.shape[1] * spec.shape[2]
    cols = spec_hbm.shape[3]
    short = rows // radix
    lines = groups // 4
    me = lax.axis_index("freq")
    core = lax.rem(me, 2)
    pair = lax.rem(me // 2, 2)
    spot = me // 4
    core_peer = me + 1 - 2 * core
    pair_peer = me + 2 - 4 * pair

    barrier = pltpu.get_barrier_semaphore()
    strips = short // 16
    tiles = cols // LANES
    small = [
        pltpu.make_async_copy(source, place, small_sem.at[i])
        for i, (source, place) in enumerate((
            (freq_hbm, freq_index), (layer_hbm, layer_ids), (slowness_hbm, slowness),
            (rays_hbm, rays), (wavelet_hbm, wavelet),
        ))
    ]
    for copy in small:
        copy.start()

    def start_load(i, carry):
        window = pl.ds(pl.multiple_of(i * 16, 16), 16)
        pltpu.make_async_copy(
            spec_hbm.at[:, :, window, :], spec.at[:, :, window, pl.ds(0, cols)], load_sem
        ).start()
        return carry

    lax.fori_loop(0, strips, start_load, 0)

    def greet(i, carry):
        pl.semaphore_signal(
            barrier, inc=1, device_id={"freq": lax.rem(me + i, groups)}, device_id_type=MESH
        )
        return carry

    with scope("greet"):
        lax.fori_loop(1, groups, greet, 0, unroll=True)

    width = cols // pieces
    deep = 32

    def x_base(strip, carry):
        k = lax.broadcasted_iota(jnp.int32, (deep, width), 0) + strip * deep
        x2 = lax.broadcasted_iota(jnp.int32, (deep, width), 1)
        sine, cosine = turn_sincos((k * x2).astype(jnp.float32) * (1.0 / width))
        row = pl.ds(pl.multiple_of(strip * deep, deep), deep)
        xbase[0, row, :] = cosine
        xbase[1, row, :] = sine
        return carry

    with scope("xbase"):
        lax.fori_loop(0, width // deep, x_base, 0, unroll=True)
    with scope("small"):
        for copy in small:
            copy.wait()

    hertz = freq_index[0].astype(jnp.float32) * (FREQUENCY_BAND / freq_total) + LOW_FREQUENCY
    angular = hertz * (2.0 * math.pi)
    slow = slowness[layer_ids[0]]
    slow_sq = slow * slow
    ray_x = rays[0]
    ray_y = rays[1]
    real_base = (angular * angular - DAMPING * DAMPING) * slow_sq
    imag_arg = 2.0 * angular * DAMPING * slow_sq
    turn_x = hertz * ray_x * GRID_STEP
    turn_y = hertz * ray_y * GRID_STEP
    vertical = jnp.full((YTALL, LANES), slow_sq - ray_x * ray_x - ray_y * ray_y, jnp.float32)
    turn_0 = jnp.sqrt(vertical) * (DEPTH_STEP * hertz)
    wave_re = wavelet[0, 0]
    wave_im = wavelet[0, 1]

    def x_first(strip, carry):
        row = pl.ds(pl.multiple_of(strip * deep, deep), deep)
        row_im = pl.ds(pl.multiple_of(strip * deep + width, deep), deep)
        cosine = xbase[0, row, :]
        sine = xbase[1, row, :]
        xtab[0, row, :] = (cosine * col_cos - sine * col_sin).astype(jnp.bfloat16)
        xtab[0, row_im, :] = (-(cosine * col_sin) - sine * col_cos).astype(jnp.bfloat16)
        return carry

    def x_table(p):
        x = lax.broadcasted_iota(jnp.int32, (deep, width), 1) * pieces + p
        x = x.astype(jnp.float32)
        away = x * turn_x
        away = away - jnp.floor(away)
        x = x * (1.0 / cols)
        k = lax.broadcasted_iota(jnp.int32, (deep, width), 0)

        def strip_of(strip, carry):
            sine, cosine = turn_sincos((k + strip * deep).astype(jnp.float32) * x + away)
            row = pl.ds(pl.multiple_of(strip * deep, deep), deep)
            row_im = pl.ds(pl.multiple_of(strip * deep + width, deep), deep)
            xtab[p, row, :] = cosine.astype(jnp.bfloat16)
            xtab[p, row_im, :] = (-sine).astype(jnp.bfloat16)
            return carry

        lax.fori_loop(0, width // deep, strip_of, 0, unroll=True)

    with scope("xt0"):
        column = lax.broadcasted_iota(jnp.int32, (8, width), 1).astype(jnp.float32) * (turn_x * pieces)
        column_sin, column_cos = turn_sincos(column)
        vecs[0, :, :width] = column_cos
        vecs[1, :, :width] = column_sin
        col_cos = vecs[0, 0:1, :width]
        col_sin = vecs[1, 0:1, :width]
        lax.fori_loop(0, width // deep, x_first, 0, unroll=True)

    ytiles = short // LANES

    tall = short // YTALL

    near_k = lax.broadcasted_iota(jnp.int32, (8, short), 1).astype(jnp.float32) * (1.0 / rows) + turn_y
    turn_sin, turn_cos = turn_sincos(lax.broadcasted_iota(jnp.int32, (8, short), 0).astype(jnp.float32) * near_k)
    vecs[0, :, :short] = turn_cos
    vecs[1, :, :short] = turn_sin

    def y_table(step, carry):
        strip = step // ytiles
        tile = lax.rem(step, ytiles)
        n2 = (lax.broadcasted_iota(jnp.int32, (YTALL, LANES), 0) + strip * YTALL).astype(jnp.float32)
        k2 = lax.broadcasted_iota(jnp.int32, (YTALL, LANES), 1) + tile * LANES
        turns = k2.astype(jnp.float32) * (n2 * (1.0 / short))
        turns = turns - jnp.floor(turns)
        sine, cosine = turn_sincos(turns + n2 * (turn_y * radix) + turn_0)
        real_0 = wave_re * cosine + wave_im * sine
        imag_0 = wave_re * sine - wave_im * cosine
        top = pl.ds(pl.multiple_of(strip * YTALL, YTALL), YTALL)
        bottom = pl.ds(pl.multiple_of(strip * YTALL + short, YTALL), YTALL)
        left = pl.ds(pl.multiple_of(tile * LANES, LANES), LANES)
        right = pl.ds(pl.multiple_of(tile * LANES + short, LANES), LANES)
        for n1 in range(radix):
            turn_re = vecs[0, n1 : n1 + 1, left]
            turn_im = vecs[1, n1 : n1 + 1, left]
            real = (real_0 * turn_re - imag_0 * turn_im).astype(jnp.bfloat16)
            imag = (real_0 * turn_im + imag_0 * turn_re).astype(jnp.bfloat16)
            ytab[n1, top, left] = real
            ytab[n1, top, right] = -imag
            ytab[n1, bottom, left] = imag
            ytab[n1, bottom, right] = real
        return carry

    with scope("ytab"):
        lax.fori_loop(0, tall * ytiles, y_table, 0, unroll=2)

    half_gain = 0.5 * DEPTH_STEP * DEPTH_STEP
    step_y = 2.0 * math.pi / (rows * GRID_STEP) * math.sqrt(half_gain)
    step_x = 2.0 * math.pi / (cols * GRID_STEP) * math.sqrt(half_gain)
    base = real_base * half_gain
    imag = imag_arg * half_gain
    imag_sq = imag * imag

    def factor(a):
        m = a * a + imag_sq
        q = m * lax.rsqrt(m) + jnp.abs(a)
        iq = lax.rsqrt(q)
        g = q * iq
        h = imag * iq
        forward = a >= 0.0
        vert_re = jnp.where(forward, g, h)
        vert_im = jnp.where(forward, h, g)
        damp = jnp.exp2(vert_im * -math.log2(math.e))
        square = vert_re * vert_re
        v = polynomial(PHASE_SIN, square) * vert_re
        w = polynomial(PHASE_COS, square)
        dv = damp * v
        return damp - dv * v, dv * w

    def signed(index, extent):
        return jnp.where(index >= extent // 2, index - extent, index).astype(jnp.float32)

    lane = lax.broadcasted_iota(jnp.int32, (8, LANES), 1)
    sub = lax.broadcasted_iota(jnp.int32, (8, LANES), 0)
    kx_sq = []
    for t in range(tiles // 2):
        kx = (lane + t * LANES).astype(jnp.float32) * step_x
        kx_sq.append(kx * kx)
    edge_x = cols // 2 * step_x
    turned = lax.rem(LANES - lane, LANES)
    flipped = lax.rem(8 - sub, 8)
    first = lane == 0
    top = sub == 0
    edge_y = (lane * 8 + sub).astype(jnp.float32) * step_y
    edge = factor(base - edge_x * edge_x - edge_y * edge_y)

    def factor_rows(m, put):
        ky = (sub + m * 8).astype(jnp.float32) * step_y
        ybase = base - ky * ky
        here = jnp.full((8, LANES), m, jnp.int32)
        after = [jnp.take_along_axis(e, here, axis=1) for e in edge]
        for t in reversed(range(tiles // 2)):
            now = factor(ybase - kx_sq[t])
            for c in range(2):
                put(c, t, now[c])
                back = jnp.take_along_axis(now[c], turned, axis=1)
                put(c, tiles - 1 - t, jnp.where(first, after[c], back))
            after = now

    middle = {}

    def put_middle(c, t, value):
        middle[c, t] = value

    def factors(i, carry):
        m = rows // 16 - 1 - i
        here = pl.ds(pl.multiple_of(m * 8, 8), 8)
        values = {}
        low = pl.ds(pl.multiple_of(rows - 8 - m * 8, 8), 8)

        def put(c, t, value):
            at = slice(t * LANES, (t + 1) * LANES)
            fac[c, low, at] = jnp.where(top, carry[c, t], jnp.take_along_axis(value, flipped, axis=0))
            fac[c, here, at] = value
            values[c, t] = value

        factor_rows(m, put)
        return values

    with scope("factors"):
        factor_rows(rows // 16, put_middle)
        lax.fori_loop(0, rows // 16, factors, middle, unroll=16)

    def shift(strip, total):
        rows_at = pl.ds(pl.multiple_of(strip * 16, 16), 16)

        def inner(tile, acc):
            at = pl.ds(pl.multiple_of(tile * LANES, LANES), LANES)
            parts = []
            for k1 in range(radix):
                row = pl.ds(pl.multiple_of(strip * 16 + k1 * short, 16), 16)
                cosine = fac[0, row, at]
                sine = fac[1, row, at]
                re = spec[0, k1, rows_at, at].astype(jnp.float32)
                im = spec[1, k1, rows_at, at].astype(jnp.float32)
                new_re = re * cosine - im * sine
                new_im = re * sine + im * cosine
                parts.append((new_re.astype(jnp.bfloat16), new_im.astype(jnp.bfloat16)))
            powers = [re * re + im * im for re, im in parts]
            while len(powers) > 1:
                powers = [x + y for x, y in zip(powers[0::2], powers[1::2])]
            acc = acc + powers[0].astype(jnp.float32)
            for n1, (re, im) in enumerate(butterfly(parts)):
                zed[n1, rows_at, at] = re
                low = pl.ds(pl.multiple_of(strip * 16 + short, 16), 16)
                zed[n1, low, at] = im
            return acc

        return lax.fori_loop(0, tiles, inner, total, unroll=8)

    with scope("shift"):
        pltpu.make_async_copy(spec_hbm, spec.at[:, :, :, pl.ds(0, cols)], load_sem).wait()
        energy = lax.fori_loop(0, strips, shift, jnp.zeros((16, LANES), jnp.float32))
    etile[...] = energy[:8] + energy[8:]

    chips = groups // 2

    def y_stage(n1, carry):
        for part in range(pieces):
            at = slice(part * width, (part + 1) * width)
            yout[part] = jnp.dot(ytab[n1], zed[n1, :, at], preferred_element_type=jnp.float32)

        def fold(strip, inner):
            top = pl.ds(pl.multiple_of(strip * 16, 16), 16)
            low = pl.ds(pl.multiple_of(strip * 16 + short, 16), 16)
            for lane_tile in range(width // LANES):
                left = slice(lane_tile * LANES, (lane_tile + 1) * LANES)
                right = slice(width + lane_tile * LANES, width + (lane_tile + 1) * LANES)
                terms = [(yout[part, top, left], yout[part, low, left]) for part in range(pieces)]
                for x1, (re, im) in enumerate(butterfly(terms)):
                    field[x1, strip, n1, :, left] = re.astype(jnp.bfloat16)
                    field[x1, strip, n1, :, right] = im.astype(jnp.bfloat16)
            return inner

        lax.fori_loop(0, chips, fold, 0, unroll=True)
        return carry

    with scope("ystage"):
        lax.fori_loop(0, radix, y_stage, 0, unroll=True)

    with scope("barr"):
        pl.semaphore_wait(barrier, groups - 1)

    def energy_copy(i):
        return pltpu.make_async_remote_copy(
            src_ref=etile, dst_ref=eall.at[i], send_sem=e_s, recv_sem=e_r,
            device_id={"freq": lax.rem(me + i, groups)}, device_id_type=MESH,
        )

    def energy_start(i, carry):
        energy_copy(i).start()
        return carry


    def ranked(j, count, centre):
        up = count - 1 - centre
        near = jnp.minimum(up, centre)
        lead = jnp.maximum(up, centre) - near
        sign = jnp.where(up >= centre, 1, -1)
        rest = jnp.maximum(j - lead, 0)
        side = jnp.where(lax.rem(rest, 2) == 0, sign, -sign)
        return jnp.where(j < lead, centre + sign * (lead + near - j), centre + side * (near - rest // 2))

    half = max(lines // 4, 1)
    blocks = lines // half
    away = (lines - 1) * pieces

    def piece(i):
        up = lines - 1 - spot
        near = jnp.minimum(up, spot)
        lead = jnp.maximum(up, spot) - near
        sign = jnp.where(up >= spot, 1, -1)
        rest = jnp.maximum(i - lead * pieces, 0)
        turn = lax.rem(rest, 2 * pieces)
        side = jnp.where(lax.rem(turn, 2) == 0, -sign, sign)
        single = i < lead * pieces
        a = jnp.where(
            single,
            spot + sign * (lead + near - i // pieces),
            spot + side * (near - rest // (2 * pieces)),
        )
        p = jnp.where(single, lax.rem(i, pieces), turn // 2)
        own = i >= away
        return jnp.where(own, spot, a), jnp.where(own, i - away, p)

    def unpaired(sender, a, p):
        beside = (a == sender + 1) | (a == sender - 1)
        inner = (a == 0) | (a == lines - 1)
        outer = ((sender == 0) | (sender == lines - 1)) & (p < SKIP)
        return beside & (inner | outer)

    def cut_of(p):
        return pl.ds(pl.multiple_of(p * width, LANES), width)

    def core_copy(block, p):
        cut = cut_of(p)
        at = pl.ds(block * half, half)
        return pltpu.make_async_remote_copy(
            src_ref=image.at[at, :, 1 - core, :, :, cut], dst_ref=core_in.at[at, :, :, :, cut],
            send_sem=core_s, recv_sem=core_r.at[block, p],
            device_id={"freq": core_peer}, device_id_type=MESH,
        )

    def pair_copy(a, p):
        cut = cut_of(p)
        return pltpu.make_async_remote_copy(
            src_ref=image.at[a, 1 - pair, core, :, :, cut], dst_ref=pair_in.at[a, :, :, cut],
            send_sem=pair_s, recv_sem=pair_r.at[a, p],
            device_id={"freq": pair_peer}, device_id_type=MESH,
        )

    def low_copy(a, p):
        cut = cut_of(p)
        return pltpu.make_async_remote_copy(
            src_ref=image.at[a, pair, core, :, :, cut], dst_ref=low_in.at[a, :, :, cut],
            send_sem=line_s, recv_sem=line_r.at[a, p],
            device_id={"freq": jnp.minimum(spot + 1, lines - 1) * 4 + pair * 2 + core},
            device_id_type=MESH,
        )

    def high_copy(a, p, arriving=False):
        cut = cut_of(p)
        return pltpu.make_async_remote_copy(
            src_ref=image.at[a, pair, core, :, :, cut], dst_ref=high_in.at[a, :, :, cut],
            send_sem=line_s, recv_sem=line_r.at[jnp.where(a == (spot if arriving else spot - 1), lines, a), p],
            device_id={"freq": jnp.maximum(spot - 1, 0) * 4 + pair * 2 + core},
            device_id_type=MESH,
        )

    def other_copy(upward, p):
        cut = cut_of(p)
        step = 1 if upward else -1
        return pltpu.make_async_remote_copy(
            src_ref=image.at[jnp.clip(spot + step, 0, lines - 1), 1 - pair, core, :, :, cut],
            dst_ref=other_in.at[0 if upward else 1, :, :, cut],
            send_sem=pair_s, recv_sem=other_r.at[0 if upward else 1, p],
            device_id={"freq": jnp.clip(spot + step, 0, lines - 1) * 4 + pair * 2 + core},
            device_id_type=MESH,
        )

    ends = (spot == 0) | (spot == lines - 1)

    def block_of(c):
        if half == 1:
            near = (lines - 2) * pieces
            moved = jnp.where(c < FIRST + SKIP, near + c - FIRST, c - SKIP)
            return piece(jnp.where(ends & (c >= FIRST) & (c < near + SKIP), moved, c))
        return ranked(c // pieces, blocks, spot // half), lax.rem(c, pieces)

    def hasty(a, p):
        return unpaired(spot, a, p) & (p < HEAD)

    def take_core(c):
        block, p = block_of(c)
        at = pl.ds(block * half, half)
        cut = cut_of(p)
        with scope("cw1"):
            core_copy(block, p).wait_recv()
        image[at, 1 - pair, core, :, :, cut] = (
            image[at, 1 - pair, core, :, :, cut] + core_in[at, 1 - pair, :, :, cut]
        )
        for h in range(half):
            a = block * half + h
            skipped = unpaired(spot, a, p)

            @pl.when(jnp.logical_not(skipped) & (a != spot))
            def _():
                pair_copy(a, p).start()

            @pl.when(skipped & (a > spot))
            def _():
                other_copy(True, p).start()

            @pl.when(skipped & (a < spot))
            def _():
                other_copy(False, p).start()

        image[at, pair, core, :, :, cut] = image[at, pair, core, :, :, cut] + core_in[at, pair, :, :, cut]
        for h in range(half):
            a = block * half + h

            @pl.when((spot == 0) & hasty(a, p))
            def _():
                low_copy(a, p).start()

            @pl.when((spot == lines - 1) & hasty(a, p))
            def _():
                high_copy(a, p).start()

    def own_start(p):
        cut = cut_of(p)

        @pl.when((spot > 0) & unpaired(spot - 1, spot, p))
        def _():
            with scope("ow"):
                other_copy(True, p).wait_recv()
            image[spot, 1 - pair, core, :, :, cut] = image[spot, 1 - pair, core, :, :, cut] + other_in[0, :, :, cut]

        @pl.when((spot < lines - 1) & unpaired(spot + 1, spot, p))
        def _():
            with scope("ow"):
                other_copy(False, p).wait_recv()
            image[spot, 1 - pair, core, :, :, cut] = image[spot, 1 - pair, core, :, :, cut] + other_in[1, :, :, cut]

        pair_copy(spot, p).start()

    lag = LAG * jnp.minimum(spot, lines - 1 - spot)

    def step(i, carry):
        a, p = piece(jnp.minimum(i, away - 1))

        @pl.when((i < away) & jnp.logical_not(unpaired(spot, a, p)))
        def _():
            cut = cut_of(p)
            with scope("yw"):
                pair_copy(a, p).wait_recv()
            image[a, pair, core, :, :, cut] = image[a, pair, core, :, :, cut] + pair_in[a, :, :, cut]

        @pl.when(i >= lag)
        def _():
            a, p = piece(jnp.clip(i - lag, 0, away - 1))
            cut = cut_of(p)

            @pl.when((a > spot) & jnp.logical_not((spot == 0) & hasty(a, p)))
            def _():
                @pl.when(spot > 0)
                def _():
                    with scope("zw"):
                        low_copy(a, p).wait_recv()
                    image[a, pair, core, :, :, cut] = image[a, pair, core, :, :, cut] + low_in[a, :, :, cut]

                low_copy(a, p).start()

            @pl.when((a < spot) & jnp.logical_not((spot == lines - 1) & hasty(a, p)))
            def _():
                @pl.when(spot < lines - 1)
                def _():
                    with scope("zw"):
                        high_copy(a, p, True).wait_recv()
                    image[a, pair, core, :, :, cut] = image[a, pair, core, :, :, cut] + high_in[a, :, :, cut]

                high_copy(a, p).start()

        @pl.when((i >= OWN) & (i < OWN + pieces))
        def _():
            own_start(i - OWN)

        return carry

    chunks = blocks * pieces

    def compute(c, carry):
        block, p = block_of(c)
        at = cut_of(p)

        with scope("dot"):
            lhs = field[p, pl.ds(2 * half * block, 2 * half)].reshape(half * 2 * radix * 16, 2 * width)
            res = jnp.dot(lhs, xtab[p], preferred_element_type=jnp.float32)
            res = res.reshape(half, 2, radix, 2, 8, width)
            for c_ in range(2):
                image[pl.ds(half * block, half), :, c_, :, :, at] = res[:, :, :, c_]
        core_copy(block, p).start()

        @pl.when(c == 0)
        def _():
            lax.fori_loop(1, groups, energy_start, 0)
            with scope("xt"):
                lax.fori_loop(1, pieces, lambda p, carry: (x_table(p), carry)[1], 0)
            take_core(c)

        @pl.when(c > BEHIND)
        def _():
            take_core(c - BEHIND)

        for i, at_chunk in enumerate(EARLY):
            @pl.when(c == min(at_chunk, chunks - 1))
            def _():
                step(i, 0)

        return carry

    with scope("compute"):
        lax.fori_loop(0, chunks, compute, 0)
        lax.fori_loop(chunks - BEHIND, chunks, lambda c, carry: (take_core(c), carry)[1], 0)

    with scope("third"):
        lax.fori_loop(len(EARLY), away + lag, step, 0)

    def all_sent(sem, ref):
        pltpu.make_async_remote_copy(
            src_ref=ref, dst_ref=ref, send_sem=sem, recv_sem=sem,
            device_id={"freq": core_peer}, device_id_type=MESH,
        ).wait_send()

    all_sent(e_r, eall.at[1:groups])

    def energy_take(i, total):
        return total + eall[i]

    total = lax.fori_loop(1, groups, energy_take, etile[...])
    total = jnp.sum(jnp.sum(total, axis=0, keepdims=True), axis=1, keepdims=True)
    scale = lax.rsqrt(total / freq_total + 1e-06)

    all_sent(e_s, eall.at[1:groups])
    all_sent(core_s, core_in)

    lanes8 = lax.broadcasted_iota(jnp.int32, (8, LANES), 1)
    part_lane = lanes8 // pieces
    lane_part = lax.rem(lanes8, pieces)

    def own(p, carry, last=False):
        cut = cut_of(p)
        with scope("oyw"):
            pair_copy(spot, p).wait_recv()
        image[spot, pair, core, :, :, cut] = image[spot, pair, core, :, :, cut] + pair_in[spot, :, :, cut]

        @pl.when(spot > 0)
        def _():
            with scope("ozw"):
                low_copy(spot, p).wait_recv()
            image[spot, pair, core, :, :, cut] = image[spot, pair, core, :, :, cut] + low_in[spot, :, :, cut]

        @pl.when(spot < lines - 1)
        def _():
            with scope("ozw"):
                high_copy(spot, p, True).wait_recv()
            image[spot, pair, core, :, :, cut] = image[spot, pair, core, :, :, cut] + high_in[spot, :, :, cut]

        for n1 in range(radix):
            for j in range(tiles):
                source = pl.ds(pl.multiple_of(p * width + j // pieces * LANES, LANES), LANES)
                value = image[spot, pair, core, n1, :, source] * scale
                spread = jnp.take_along_axis(value, part_lane + j % pieces * (LANES // pieces), axis=1)
                to = slice(j * LANES, (j + 1) * LANES)
                mine = jnp.where(lane_part == p, spread, mixed[n1, :, to])

                if last:
                    out_ref[:, n1, to] = mine
                else:
                    mixed[n1, :, to] = mine
        return carry

    with scope("own"):
        lax.fori_loop(0, pieces - 1, own, 0)
        own(pieces - 1, 0, last=True)

    with scope("ownend"):
        all_sent(line_s, pair_in.at[1:lines])
        all_sent(pair_s, pair_in)


def body(spectra, wavelet, freq_index, slowness, layer_ids, ray_slowness):
    slot_total, unused, rows, cols = spectra.shape
    groups = lax.axis_size("freq")
    freq_total = slot_total * groups
    radix = rows // groups // 8
    short = rows // radix
    lines = groups // 4
    pieces = min(4, cols // LANES)
    f32, bf16 = jnp.float32, jnp.bfloat16
    dma = pltpu.SemaphoreType.DMA
    out = pl.pallas_call(
        functools.partial(kernel, groups, radix, pieces, freq_total),
        out_shape=pltpu.VMEM((8, radix, cols), f32),
        in_specs=[
            *[pl.BlockSpec(memory_space=pl.ANY)] * 6,
        ],
        out_specs=pl.BlockSpec(memory_space=pltpu.VMEM),
        scratch_shapes=[
            *[pltpu.SMEM(small.shape, small.dtype) for small in (wavelet, freq_index, slowness, layer_ids, ray_slowness)],
            pltpu.VMEM((2, radix, short, cols + LANES), bf16),
            pltpu.VMEM((radix, 2 * short, cols + LANES), bf16),
            pltpu.VMEM((radix, 2 * short, 2 * short), bf16),
            pltpu.VMEM((pieces, groups // 2, radix, 16, 2 * (cols // pieces)), bf16),
            pltpu.VMEM((pieces, 2 * (cols // pieces), cols // pieces), bf16),
            pltpu.VMEM((pieces, 2 * short, cols // pieces), f32),
            pltpu.VMEM((2, 8, max(short, cols // pieces)), f32),
            pltpu.VMEM((2, cols // pieces, cols // pieces), f32),
            pltpu.VMEM((2, rows + 8, cols + LANES), f32),
            pltpu.VMEM((radix, 8, cols), f32),
            pltpu.VMEM((lines, 2, 2, radix, 8, cols), f32),
            pltpu.VMEM((lines, 2, radix, 8, cols), f32),
            pltpu.VMEM((lines, radix, 8, cols), f32),
            pltpu.VMEM((lines, radix, 8, cols), f32),
            pltpu.VMEM((lines, radix, 8, cols), f32),
            pltpu.VMEM((2, radix, 8, cols), f32),
            pltpu.VMEM((8, LANES), f32),
            pltpu.VMEM((groups, 8, LANES), f32),
            dma((5,)),
            dma,
            dma,
            dma((min(lines, 4), pieces)),
            dma,
            dma((lines, pieces)),
            dma,
            dma((lines + 1, pieces)),
            dma((2, pieces)),
            dma,
            dma,
        ],
        compiler_params=pltpu.CompilerParams(
            collective_id=0, has_side_effects=True, vmem_limit_bytes=60 * 1024 * 1024
        ),
    )(
        wavelet, freq_index, slowness, layer_ids, ray_slowness,
        spectra.reshape(2, radix, short, cols),
    )
    return out.reshape(1, 8 * radix, cols)


def solution(mesh):
    placed = (
        P(("rays", "freq"), None, None, None),
        P("freq", None),
        P("freq"),
        P(),
        P(),
        P("rays"),
    )
    return jax.shard_map(
        body, mesh=mesh, in_specs=placed, out_specs=P("rays", "freq", None), check_vma=False
    )
```

```python
import contextlib
import functools
import math

import jax
import jax.numpy as jnp
from jax import lax
from jax.experimental import pallas as pl
from jax.experimental.pallas import tpu as pltpu
from jax.sharding import PartitionSpec as P

GRID_STEP = 12.5
DEPTH_STEP = 10.0
LOW_FREQUENCY = 5.0
FREQUENCY_BAND = 50.0
DAMPING = 6.0
LANES = 128
LAG = 2
BEHIND = 3
SKIP = 2
FIRST = 2
HEAD = 1
EARLY = (11, 14)
OWN = 4
YTALL = 64
MESH = pl.DeviceIdType.MESH

HALF_SIN = (0.9999998807907104, -0.16666465997695923, 0.008326363749802113, -0.00019062065985053778)
HALF_COS = (0.9999992251396179, -0.499982088804245, 0.04160428047180176, -0.0013190462486818433)
TURN_SIN = (0.9999992251396179, -0.16665679216384888, 0.008313224650919437, -0.0001852344867074862)
TURN_COS = (
    0.9999999403953552, -0.4999990463256836, 0.041663579642772675, -0.0013853666605427861,
    2.315317397005856e-05,
)

ROOT = math.sqrt(2.0)
PHASE_SIN = tuple(ROOT * c / 2.0 ** (2 * k + 1) for k, c in enumerate(HALF_SIN))
PHASE_COS = tuple(ROOT * c / 4.0**k for k, c in enumerate(HALF_COS))


def scope(name):
    return contextlib.nullcontext()


def polynomial(coefs, square):
    value = square * coefs[-1] + coefs[-2]
    for coef in coefs[-3::-1]:
        value = value * square + coef
    return value


def half_sincos(half, sin_coefs, cos_coefs):
    square = half * half
    sine = polynomial(sin_coefs, square) * half
    twice = sine + sine
    return twice * polynomial(cos_coefs, square), 1.0 - twice * sine


def turn_sincos(turns):
    reduced = turns - jnp.floor(turns + 0.5)
    return half_sincos(reduced * math.pi, TURN_SIN, TURN_COS)


def butterfly(parts):
    count = len(parts)
    if count == 1:
        return parts
    even = butterfly(parts[0::2])
    odd = butterfly(parts[1::2])
    low, high = [], []
    for i in range(count // 2):
        er, ei = even[i]
        xr, xi = odd[i]
        if i == 0:
            tr, ti = xr, xi
        elif 4 * i == count:
            tr, ti = -xi, xr
        elif 8 * i == count:
            root = math.sqrt(0.5)
            tr, ti = (xr - xi) * root, (xr + xi) * root
        elif 8 * i == 3 * count:
            root = math.sqrt(0.5)
            tr, ti = (xr + xi) * -root, (xr - xi) * root
        else:
            c = math.cos(2 * math.pi * i / count)
            s = math.sin(2 * math.pi * i / count)
            tr, ti = xr * c - xi * s, xr * s + xi * c
        low.append((er + tr, ei + ti))
        high.append((er - tr, ei - ti))
    return low + high


def kernel(
    groups, radix, pieces, freq_total,
    wavelet_hbm, freq_hbm, slowness_hbm, layer_hbm, rays_hbm, spec_hbm, out_ref,
    wavelet, freq_index, slowness, layer_ids, rays,
    spec, zed_a, zed_b, ytab, field, xtab, yout, vecs, xbase, fac, mixed, image, core_in, pair_in, low_in, high_in, other_in, etile, eall,
    small_sem, load_sem, core_s, core_r, pair_s, pair_r, line_s, line_r, other_r, e_s, e_r,
):
    rows = spec.shape[1] * spec.shape[2]
    cols = spec_hbm.shape[3]
    short = rows // radix
    lines = groups // 4
    me = lax.axis_index("freq")
    core = lax.rem(me, 2)
    pair = lax.rem(me // 2, 2)
    spot = me // 4
    core_peer = me + 1 - 2 * core
    pair_peer = me + 2 - 4 * pair

    barrier = pltpu.get_barrier_semaphore()
    strips = short // 16
    tiles = cols // LANES
    small = [
        pltpu.make_async_copy(source, place, small_sem.at[i])
        for i, (source, place) in enumerate((
            (freq_hbm, freq_index), (layer_hbm, layer_ids), (slowness_hbm, slowness),
            (rays_hbm, rays), (wavelet_hbm, wavelet),
        ))
    ]
    for copy in small:
        copy.start()

    def start_load(i, carry):
        window = pl.ds(pl.multiple_of(i * 16, 16), 16)
        pltpu.make_async_copy(
            spec_hbm.at[:, :, window, :], spec.at[:, :, window, pl.ds(0, cols)], load_sem
        ).start()
        return carry

    lax.fori_loop(0, strips, start_load, 0)

    def greet(i, carry):
        pl.semaphore_signal(
            barrier, inc=1, device_id={"freq": lax.rem(me + i, groups)}, device_id_type=MESH
        )
        return carry

    with scope("greet"):
        lax.fori_loop(1, groups, greet, 0, unroll=True)

    width = cols // pieces
    deep = 32

    def x_base(strip, carry):
        k = lax.broadcasted_iota(jnp.int32, (deep, width), 0) + strip * deep
        x2 = lax.broadcasted_iota(jnp.int32, (deep, width), 1)
        sine, cosine = turn_sincos((k * x2).astype(jnp.float32) * (1.0 / width))
        row = pl.ds(pl.multiple_of(strip * deep, deep), deep)
        xbase[0, row, :] = cosine
        xbase[1, row, :] = sine
        return carry

    with scope("xbase"):
        lax.fori_loop(0, width // deep, x_base, 0, unroll=True)
    with scope("small"):
        for copy in small:
            copy.wait()

    hertz = freq_index[0].astype(jnp.float32) * (FREQUENCY_BAND / freq_total) + LOW_FREQUENCY
    angular = hertz * (2.0 * math.pi)
    slow = slowness[layer_ids[0]]
    slow_sq = slow * slow
    ray_x = rays[0]
    ray_y = rays[1]
    real_base = (angular * angular - DAMPING * DAMPING) * slow_sq
    imag_arg = 2.0 * angular * DAMPING * slow_sq
    turn_x = hertz * ray_x * GRID_STEP
    turn_y = hertz * ray_y * GRID_STEP
    vertical = jnp.full((YTALL, LANES), slow_sq - ray_x * ray_x - ray_y * ray_y, jnp.float32)
    turn_0 = jnp.sqrt(vertical) * (DEPTH_STEP * hertz)
    wave_re = wavelet[0, 0]
    wave_im = wavelet[0, 1]

    def x_first(strip, carry):
        row = pl.ds(pl.multiple_of(strip * deep, deep), deep)
        row_im = pl.ds(pl.multiple_of(strip * deep + width, deep), deep)
        cosine = xbase[0, row, :]
        sine = xbase[1, row, :]
        xtab[0, row, :] = (cosine * col_cos - sine * col_sin).astype(jnp.bfloat16)
        xtab[0, row_im, :] = (-(cosine * col_sin) - sine * col_cos).astype(jnp.bfloat16)
        return carry

    def x_table(p):
        x = lax.broadcasted_iota(jnp.int32, (deep, width), 1) * pieces + p
        x = x.astype(jnp.float32)
        away = x * turn_x
        away = away - jnp.floor(away)
        x = x * (1.0 / cols)
        k = lax.broadcasted_iota(jnp.int32, (deep, width), 0)

        def strip_of(strip, carry):
            sine, cosine = turn_sincos((k + strip * deep).astype(jnp.float32) * x + away)
            row = pl.ds(pl.multiple_of(strip * deep, deep), deep)
            row_im = pl.ds(pl.multiple_of(strip * deep + width, deep), deep)
            xtab[p, row, :] = cosine.astype(jnp.bfloat16)
            xtab[p, row_im, :] = (-sine).astype(jnp.bfloat16)
            return carry

        lax.fori_loop(0, width // deep, strip_of, 0, unroll=True)

    with scope("xt0"):
        column = lax.broadcasted_iota(jnp.int32, (8, width), 1).astype(jnp.float32) * (turn_x * pieces)
        column_sin, column_cos = turn_sincos(column)
        vecs[0, :, :width] = column_cos
        vecs[1, :, :width] = column_sin
        col_cos = vecs[0, 0:1, :width]
        col_sin = vecs[1, 0:1, :width]
        lax.fori_loop(0, width // deep, x_first, 0, unroll=True)

    ytiles = short // LANES

    tall = short // YTALL

    near_k = lax.broadcasted_iota(jnp.int32, (8, short), 1).astype(jnp.float32) * (1.0 / rows) + turn_y
    turn_sin, turn_cos = turn_sincos(lax.broadcasted_iota(jnp.int32, (8, short), 0).astype(jnp.float32) * near_k)
    vecs[0, :, :short] = turn_cos
    vecs[1, :, :short] = turn_sin

    def y_table(step, carry):
        strip = step // ytiles
        tile = lax.rem(step, ytiles)
        n2 = (lax.broadcasted_iota(jnp.int32, (YTALL, LANES), 0) + strip * YTALL).astype(jnp.float32)
        k2 = lax.broadcasted_iota(jnp.int32, (YTALL, LANES), 1) + tile * LANES
        turns = k2.astype(jnp.float32) * (n2 * (1.0 / short))
        turns = turns - jnp.floor(turns)
        sine, cosine = turn_sincos(turns + n2 * (turn_y * radix) + turn_0)
        real_0 = wave_re * cosine + wave_im * sine
        imag_0 = wave_re * sine - wave_im * cosine
        top = pl.ds(pl.multiple_of(strip * YTALL, YTALL), YTALL)
        bottom = pl.ds(pl.multiple_of(strip * YTALL + short, YTALL), YTALL)
        left = pl.ds(pl.multiple_of(tile * LANES, LANES), LANES)
        right = pl.ds(pl.multiple_of(tile * LANES + short, LANES), LANES)
        for n1 in range(radix):
            turn_re = vecs[0, n1 : n1 + 1, left]
            turn_im = vecs[1, n1 : n1 + 1, left]
            real = (real_0 * turn_re - imag_0 * turn_im).astype(jnp.bfloat16)
            imag = (real_0 * turn_im + imag_0 * turn_re).astype(jnp.bfloat16)
            ytab[n1, top, left] = real
            ytab[n1, top, right] = -imag
            ytab[n1, bottom, left] = imag
            ytab[n1, bottom, right] = real
        return carry

    with scope("ytab"):
        lax.fori_loop(0, tall * ytiles, y_table, 0, unroll=2)

    half_gain = 0.5 * DEPTH_STEP * DEPTH_STEP
    step_y = 2.0 * math.pi / (rows * GRID_STEP) * math.sqrt(half_gain)
    step_x = 2.0 * math.pi / (cols * GRID_STEP) * math.sqrt(half_gain)
    base = real_base * half_gain
    imag = imag_arg * half_gain
    imag_sq = imag * imag

    def factor(a):
        m = a * a + imag_sq
        q = m * lax.rsqrt(m) + jnp.abs(a)
        iq = lax.rsqrt(q)
        g = q * iq
        h = imag * iq
        forward = a >= 0.0
        vert_re = jnp.where(forward, g, h)
        vert_im = jnp.where(forward, h, g)
        damp = jnp.exp2(vert_im * -math.log2(math.e))
        square = vert_re * vert_re
        v = polynomial(PHASE_SIN, square) * vert_re
        w = polynomial(PHASE_COS, square)
        dv = damp * v
        return damp - dv * v, dv * w

    def signed(index, extent):
        return jnp.where(index >= extent // 2, index - extent, index).astype(jnp.float32)

    lane = lax.broadcasted_iota(jnp.int32, (8, LANES), 1)
    sub = lax.broadcasted_iota(jnp.int32, (8, LANES), 0)
    kx_sq = []
    for t in range(tiles // 2):
        kx = (lane + t * LANES).astype(jnp.float32) * step_x
        kx_sq.append(kx * kx)
    edge_x = cols // 2 * step_x
    turned = lax.rem(LANES - lane, LANES)
    flipped = lax.rem(8 - sub, 8)
    first = lane == 0
    top = sub == 0
    edge_y = (lane * 8 + sub).astype(jnp.float32) * step_y
    edge = factor(base - edge_x * edge_x - edge_y * edge_y)

    def factor_rows(m, put):
        ky = (sub + m * 8).astype(jnp.float32) * step_y
        ybase = base - ky * ky
        here = jnp.full((8, LANES), m, jnp.int32)
        after = [jnp.take_along_axis(e, here, axis=1) for e in edge]
        for t in reversed(range(tiles // 2)):
            now = factor(ybase - kx_sq[t])
            for c in range(2):
                put(c, t, now[c])
                back = jnp.take_along_axis(now[c], turned, axis=1)
                put(c, tiles - 1 - t, jnp.where(first, after[c], back))
            after = now

    middle = {}

    def put_middle(c, t, value):
        middle[c, t] = value

    def factors(i, carry):
        m = rows // 16 - 1 - i
        here = pl.ds(pl.multiple_of(m * 8, 8), 8)
        values = {}
        low = pl.ds(pl.multiple_of(rows - 8 - m * 8, 8), 8)

        def put(c, t, value):
            at = slice(t * LANES, (t + 1) * LANES)
            fac[c, low, at] = jnp.where(top, carry[c, t], jnp.take_along_axis(value, flipped, axis=0))
            fac[c, here, at] = value
            values[c, t] = value

        factor_rows(m, put)
        return values

    with scope("factors"):
        factor_rows(rows // 16, put_middle)
        lax.fori_loop(0, rows // 16, factors, middle, unroll=16)

    chips = groups // 2
    half_width = width // 2
    spread = half_width * pieces

    def shift(strip, half_at, zed, acc):
        rows_at = pl.ds(pl.multiple_of(strip * 16, 16), 16)
        low = pl.ds(pl.multiple_of(strip * 16 + short, 16), 16)
        for tile in range(spread // LANES):
            part, column = divmod(tile * LANES, half_width)
            column = part * width + half_at * half_width + column
            at = slice(column, column + LANES)
            to = slice(tile * LANES, (tile + 1) * LANES)
            parts = []
            for k1 in range(radix):
                row = pl.ds(pl.multiple_of(strip * 16 + k1 * short, 16), 16)
                cosine = fac[0, row, at]
                sine = fac[1, row, at]
                re = spec[0, k1, rows_at, at].astype(jnp.float32)
                im = spec[1, k1, rows_at, at].astype(jnp.float32)
                new_re = re * cosine - im * sine
                new_im = re * sine + im * cosine
                parts.append((new_re.astype(jnp.bfloat16), new_im.astype(jnp.bfloat16)))
            powers = [re * re + im * im for re, im in parts]
            while len(powers) > 1:
                powers = [x + y for x, y in zip(powers[0::2], powers[1::2])]
            acc = acc + powers[0].astype(jnp.float32)
            for n1, (re, im) in enumerate(butterfly(parts)):
                zed[n1, rows_at, to] = re
                zed[n1, low, to] = im
        return acc

    def y_stage(n1, half_at, zed):
        slot = n1 % 2
        for start in range(0, spread, 256):
            at = slice(start, start + 256)
            yout[slot, :, at] = jnp.dot(ytab[n1], zed[n1, :, at], preferred_element_type=jnp.float32)

        def fold(strip, inner):
            top = pl.ds(pl.multiple_of(strip * 16, 16), 16)
            low = pl.ds(pl.multiple_of(strip * 16 + short, 16), 16)
            for column in range(0, half_width, LANES):
                left = slice(half_at * half_width + column, half_at * half_width + column + LANES)
                right = slice(left.start + width, left.stop + width)
                terms = []
                for part in range(pieces):
                    of = slice(part * half_width + column, part * half_width + column + LANES)
                    terms.append((yout[slot, top, of], yout[slot, low, of]))
                for x1, (re, im) in enumerate(butterfly(terms)):
                    field[x1, strip, n1, :, left] = re.astype(jnp.bfloat16)
                    field[x1, strip, n1, :, right] = im.astype(jnp.bfloat16)
            return inner

        lax.fori_loop(0, chips, fold, 0, unroll=True)

    energy = jnp.zeros((16, LANES), jnp.float32)
    with scope("shift"):
        pltpu.make_async_copy(spec_hbm, spec.at[:, :, :, pl.ds(0, cols)], load_sem).wait()
        energy = lax.fori_loop(0, strips, lambda i, acc: shift(i, 0, zed_a, acc), energy, unroll=2)
    with scope("both"):
        share = strips // radix
        for n1 in range(radix):
            energy = lax.fori_loop(
                n1 * share, (n1 + 1) * share, lambda i, acc: shift(i, 1, zed_b, acc), energy, unroll=share == 1
            )
            y_stage(n1, 0, zed_a)
    etile[...] = energy[:8] + energy[8:]

    with scope("ystage"):
        for n1 in range(radix):
            y_stage(n1, 1, zed_b)

    with scope("barr"):
        pl.semaphore_wait(barrier, groups - 1)

    def energy_copy(i):
        return pltpu.make_async_remote_copy(
            src_ref=etile, dst_ref=eall.at[i], send_sem=e_s, recv_sem=e_r,
            device_id={"freq": lax.rem(me + i, groups)}, device_id_type=MESH,
        )

    def energy_start(i, carry):
        energy_copy(i).start()
        return carry


    def ranked(j, count, centre):
        up = count - 1 - centre
        near = jnp.minimum(up, centre)
        lead = jnp.maximum(up, centre) - near
        sign = jnp.where(up >= centre, 1, -1)
        rest = jnp.maximum(j - lead, 0)
        side = jnp.where(lax.rem(rest, 2) == 0, sign, -sign)
        return jnp.where(j < lead, centre + sign * (lead + near - j), centre + side * (near - rest // 2))

    half = max(lines // 4, 1)
    blocks = lines // half
    away = (lines - 1) * pieces

    def piece(i):
        up = lines - 1 - spot
        near = jnp.minimum(up, spot)
        lead = jnp.maximum(up, spot) - near
        sign = jnp.where(up >= spot, 1, -1)
        rest = jnp.maximum(i - lead * pieces, 0)
        turn = lax.rem(rest, 2 * pieces)
        side = jnp.where(lax.rem(turn, 2) == 0, -sign, sign)
        single = i < lead * pieces
        a = jnp.where(
            single,
            spot + sign * (lead + near - i // pieces),
            spot + side * (near - rest // (2 * pieces)),
        )
        p = jnp.where(single, lax.rem(i, pieces), turn // 2)
        own = i >= away
        return jnp.where(own, spot, a), jnp.where(own, i - away, p)

    def unpaired(sender, a, p):
        beside = (a == sender + 1) | (a == sender - 1)
        inner = (a == 0) | (a == lines - 1)
        outer = ((sender == 0) | (sender == lines - 1)) & (p < SKIP)
        return beside & (inner | outer)

    def cut_of(p):
        return pl.ds(pl.multiple_of(p * width, LANES), width)

    def core_copy(block, p):
        cut = cut_of(p)
        at = pl.ds(block * half, half)
        return pltpu.make_async_remote_copy(
            src_ref=image.at[at, :, 1 - core, :, :, cut], dst_ref=core_in.at[at, :, :, :, cut],
            send_sem=core_s, recv_sem=core_r.at[block, p],
            device_id={"freq": core_peer}, device_id_type=MESH,
        )

    def pair_copy(a, p):
        cut = cut_of(p)
        return pltpu.make_async_remote_copy(
            src_ref=image.at[a, 1 - pair, core, :, :, cut], dst_ref=pair_in.at[a, :, :, cut],
            send_sem=pair_s, recv_sem=pair_r.at[a, p],
            device_id={"freq": pair_peer}, device_id_type=MESH,
        )

    def low_copy(a, p):
        cut = cut_of(p)
        return pltpu.make_async_remote_copy(
            src_ref=image.at[a, pair, core, :, :, cut], dst_ref=low_in.at[a, :, :, cut],
            send_sem=line_s, recv_sem=line_r.at[a, p],
            device_id={"freq": jnp.minimum(spot + 1, lines - 1) * 4 + pair * 2 + core},
            device_id_type=MESH,
        )

    def high_copy(a, p, arriving=False):
        cut = cut_of(p)
        return pltpu.make_async_remote_copy(
            src_ref=image.at[a, pair, core, :, :, cut], dst_ref=high_in.at[a, :, :, cut],
            send_sem=line_s, recv_sem=line_r.at[jnp.where(a == (spot if arriving else spot - 1), lines, a), p],
            device_id={"freq": jnp.maximum(spot - 1, 0) * 4 + pair * 2 + core},
            device_id_type=MESH,
        )

    def other_copy(upward, p):
        cut = cut_of(p)
        step = 1 if upward else -1
        return pltpu.make_async_remote_copy(
            src_ref=image.at[jnp.clip(spot + step, 0, lines - 1), 1 - pair, core, :, :, cut],
            dst_ref=other_in.at[0 if upward else 1, :, :, cut],
            send_sem=pair_s, recv_sem=other_r.at[0 if upward else 1, p],
            device_id={"freq": jnp.clip(spot + step, 0, lines - 1) * 4 + pair * 2 + core},
            device_id_type=MESH,
        )

    ends = (spot == 0) | (spot == lines - 1)

    def block_of(c):
        if half == 1:
            near = (lines - 2) * pieces
            moved = jnp.where(c < FIRST + SKIP, near + c - FIRST, c - SKIP)
            return piece(jnp.where(ends & (c >= FIRST) & (c < near + SKIP), moved, c))
        return ranked(c // pieces, blocks, spot // half), lax.rem(c, pieces)

    def hasty(a, p):
        return unpaired(spot, a, p) & (p < HEAD)

    def take_core(c):
        block, p = block_of(c)
        at = pl.ds(block * half, half)
        cut = cut_of(p)
        with scope("cw1"):
            core_copy(block, p).wait_recv()
        image[at, 1 - pair, core, :, :, cut] = (
            image[at, 1 - pair, core, :, :, cut] + core_in[at, 1 - pair, :, :, cut]
        )
        for h in range(half):
            a = block * half + h
            skipped = unpaired(spot, a, p)

            @pl.when(jnp.logical_not(skipped) & (a != spot))
            def _():
                pair_copy(a, p).start()

            @pl.when(skipped & (a > spot))
            def _():
                other_copy(True, p).start()

            @pl.when(skipped & (a < spot))
            def _():
                other_copy(False, p).start()

        image[at, pair, core, :, :, cut] = image[at, pair, core, :, :, cut] + core_in[at, pair, :, :, cut]
        for h in range(half):
            a = block * half + h

            @pl.when((spot == 0) & hasty(a, p))
            def _():
                low_copy(a, p).start()

            @pl.when((spot == lines - 1) & hasty(a, p))
            def _():
                high_copy(a, p).start()

    def own_start(p):
        cut = cut_of(p)

        @pl.when((spot > 0) & unpaired(spot - 1, spot, p))
        def _():
            with scope("ow"):
                other_copy(True, p).wait_recv()
            image[spot, 1 - pair, core, :, :, cut] = image[spot, 1 - pair, core, :, :, cut] + other_in[0, :, :, cut]

        @pl.when((spot < lines - 1) & unpaired(spot + 1, spot, p))
        def _():
            with scope("ow"):
                other_copy(False, p).wait_recv()
            image[spot, 1 - pair, core, :, :, cut] = image[spot, 1 - pair, core, :, :, cut] + other_in[1, :, :, cut]

        pair_copy(spot, p).start()

    lag = LAG * jnp.minimum(spot, lines - 1 - spot)

    def step(i, carry):
        a, p = piece(jnp.minimum(i, away - 1))

        @pl.when((i < away) & jnp.logical_not(unpaired(spot, a, p)))
        def _():
            cut = cut_of(p)
            with scope("yw"):
                pair_copy(a, p).wait_recv()
            image[a, pair, core, :, :, cut] = image[a, pair, core, :, :, cut] + pair_in[a, :, :, cut]

        @pl.when(i >= lag)
        def _():
            a, p = piece(jnp.clip(i - lag, 0, away - 1))
            cut = cut_of(p)

            @pl.when((a > spot) & jnp.logical_not((spot == 0) & hasty(a, p)))
            def _():
                @pl.when(spot > 0)
                def _():
                    with scope("zw"):
                        low_copy(a, p).wait_recv()
                    image[a, pair, core, :, :, cut] = image[a, pair, core, :, :, cut] + low_in[a, :, :, cut]

                low_copy(a, p).start()

            @pl.when((a < spot) & jnp.logical_not((spot == lines - 1) & hasty(a, p)))
            def _():
                @pl.when(spot < lines - 1)
                def _():
                    with scope("zw"):
                        high_copy(a, p, True).wait_recv()
                    image[a, pair, core, :, :, cut] = image[a, pair, core, :, :, cut] + high_in[a, :, :, cut]

                high_copy(a, p).start()

        @pl.when((i >= OWN) & (i < OWN + pieces))
        def _():
            own_start(i - OWN)

        return carry

    chunks = blocks * pieces

    def compute(c, carry):
        block, p = block_of(c)
        at = cut_of(p)

        with scope("dot"):
            lhs = field[p, pl.ds(2 * half * block, 2 * half)].reshape(half * 2 * radix * 16, 2 * width)
            res = jnp.dot(lhs, xtab[p], preferred_element_type=jnp.float32)
            res = res.reshape(half, 2, radix, 2, 8, width)
            for c_ in range(2):
                image[pl.ds(half * block, half), :, c_, :, :, at] = res[:, :, :, c_]
        core_copy(block, p).start()

        @pl.when(c == 0)
        def _():
            lax.fori_loop(1, groups, energy_start, 0)
            with scope("xt"):
                lax.fori_loop(1, pieces, lambda p, carry: (x_table(p), carry)[1], 0)
            take_core(c)

        @pl.when(c > BEHIND)
        def _():
            take_core(c - BEHIND)

        for i, at_chunk in enumerate(EARLY):
            @pl.when(c == min(at_chunk, chunks - 1))
            def _():
                step(i, 0)

        return carry

    with scope("compute"):
        lax.fori_loop(0, chunks, compute, 0)
        lax.fori_loop(chunks - BEHIND, chunks, lambda c, carry: (take_core(c), carry)[1], 0)

    with scope("third"):
        lax.fori_loop(len(EARLY), away + lag, step, 0)

    def all_sent(sem, ref):
        pltpu.make_async_remote_copy(
            src_ref=ref, dst_ref=ref, send_sem=sem, recv_sem=sem,
            device_id={"freq": core_peer}, device_id_type=MESH,
        ).wait_send()

    all_sent(e_r, eall.at[1:groups])

    def energy_take(i, total):
        return total + eall[i]

    total = lax.fori_loop(1, groups, energy_take, etile[...])
    total = jnp.sum(jnp.sum(total, axis=0, keepdims=True), axis=1, keepdims=True)
    scale = lax.rsqrt(total / freq_total + 1e-06)

    all_sent(e_s, eall.at[1:groups])
    all_sent(core_s, core_in)

    lanes8 = lax.broadcasted_iota(jnp.int32, (8, LANES), 1)
    part_lane = lanes8 // pieces
    lane_part = lax.rem(lanes8, pieces)

    def own(p, carry, last=False):
        cut = cut_of(p)
        with scope("oyw"):
            pair_copy(spot, p).wait_recv()
        image[spot, pair, core, :, :, cut] = image[spot, pair, core, :, :, cut] + pair_in[spot, :, :, cut]

        @pl.when(spot > 0)
        def _():
            with scope("ozw"):
                low_copy(spot, p).wait_recv()
            image[spot, pair, core, :, :, cut] = image[spot, pair, core, :, :, cut] + low_in[spot, :, :, cut]

        @pl.when(spot < lines - 1)
        def _():
            with scope("ozw"):
                high_copy(spot, p, True).wait_recv()
            image[spot, pair, core, :, :, cut] = image[spot, pair, core, :, :, cut] + high_in[spot, :, :, cut]

        for n1 in range(radix):
            for j in range(tiles):
                source = pl.ds(pl.multiple_of(p * width + j // pieces * LANES, LANES), LANES)
                value = image[spot, pair, core, n1, :, source] * scale
                spread = jnp.take_along_axis(value, part_lane + j % pieces * (LANES // pieces), axis=1)
                to = slice(j * LANES, (j + 1) * LANES)
                mine = jnp.where(lane_part == p, spread, mixed[n1, :, to])

                if last:
                    out_ref[:, n1, to] = mine
                else:
                    mixed[n1, :, to] = mine
        return carry

    with scope("own"):
        lax.fori_loop(0, pieces - 1, own, 0)
        own(pieces - 1, 0, last=True)

    with scope("ownend"):
        all_sent(line_s, pair_in.at[1:lines])
        all_sent(pair_s, pair_in)


def body(spectra, wavelet, freq_index, slowness, layer_ids, ray_slowness):
    slot_total, unused, rows, cols = spectra.shape
    groups = lax.axis_size("freq")
    freq_total = slot_total * groups
    radix = rows // groups // 8
    short = rows // radix
    lines = groups // 4
    pieces = min(4, cols // LANES)
    f32, bf16 = jnp.float32, jnp.bfloat16
    dma = pltpu.SemaphoreType.DMA
    out = pl.pallas_call(
        functools.partial(kernel, groups, radix, pieces, freq_total),
        out_shape=pltpu.VMEM((8, radix, cols), f32),
        in_specs=[
            *[pl.BlockSpec(memory_space=pl.ANY)] * 6,
        ],
        out_specs=pl.BlockSpec(memory_space=pltpu.VMEM),
        scratch_shapes=[
            *[pltpu.SMEM(small.shape, small.dtype) for small in (wavelet, freq_index, slowness, layer_ids, ray_slowness)],
            pltpu.VMEM((2, radix, short, cols + LANES), bf16),
            pltpu.VMEM((radix, 2 * short, cols // 2 + LANES), bf16),
            pltpu.VMEM((radix, 2 * short, cols // 2 + LANES), bf16),
            pltpu.VMEM((radix, 2 * short, 2 * short), bf16),
            pltpu.VMEM((pieces, groups // 2, radix, 16, 2 * (cols // pieces)), bf16),
            pltpu.VMEM((pieces, 2 * (cols // pieces), cols // pieces), bf16),
            pltpu.VMEM((2, 2 * short, cols // 2), f32),
            pltpu.VMEM((2, 8, max(short, cols // pieces)), f32),
            pltpu.VMEM((2, cols // pieces, cols // pieces), f32),
            pltpu.VMEM((2, rows + 8, cols + LANES), f32),
            pltpu.VMEM((radix, 8, cols), f32),
            pltpu.VMEM((lines, 2, 2, radix, 8, cols), f32),
            pltpu.VMEM((lines, 2, radix, 8, cols), f32),
            pltpu.VMEM((lines, radix, 8, cols), f32),
            pltpu.VMEM((lines, radix, 8, cols), f32),
            pltpu.VMEM((lines, radix, 8, cols), f32),
            pltpu.VMEM((2, radix, 8, cols), f32),
            pltpu.VMEM((8, LANES), f32),
            pltpu.VMEM((groups, 8, LANES), f32),
            dma((5,)),
            dma,
            dma,
            dma((min(lines, 4), pieces)),
            dma,
            dma((lines, pieces)),
            dma,
            dma((lines + 1, pieces)),
            dma((2, pieces)),
            dma,
            dma,
        ],
        compiler_params=pltpu.CompilerParams(
            collective_id=0, has_side_effects=True, vmem_limit_bytes=60 * 1024 * 1024
        ),
    )(
        wavelet, freq_index, slowness, layer_ids, ray_slowness,
        spectra.reshape(2, radix, short, cols),
    )
    return out.reshape(1, 8 * radix, cols)


def solution(mesh):
    placed = (
        P(("rays", "freq"), None, None, None),
        P("freq", None),
        P("freq"),
        P(),
        P(),
        P("rays"),
    )
    return jax.shard_map(
        body, mesh=mesh, in_specs=placed, out_specs=P("rays", "freq", None), check_vma=False
    )
```
